512 devices in a mesh: beam: 16 (over z), pulse: 4 (over x), range: 8 (over y, core).
Axes of the slice: x: 4, y: 4, z: 16, core: 2. Of those that a mesh axis runs over, the one named last changes fastest.
Arguments:
- signal: bfloat16 [32, 32, 2, 4096], P('beam', 'pulse', None, 'range'), may hold values from -40 to 40, as said below
- replica: bfloat16 [2, 2048], P(None, ('beam', 'pulse')), may hold values from -0.09375 to 0.09375
- guard_cells: int32 [32], P('beam'), may hold values from 1 to 8, as said below
- train_cells: int32 [32], P('beam'), may hold values from 64 to 96, as said below
- scale_index: int32 [32], P('beam'), may hold values from 0 to 15
- offsets: int32 [32], P('beam'), may hold values from 0 to 127, as said below
Outputs:
- compressed: bfloat16 [32, 32, 2, 4096], P('beam', 'pulse', None, 'range')
- test_ratio: float32 [32, 32, 4096], P('beam', 'pulse', 'range')
The draws below stay inside these ranges and needn't reach their ends.
Inputs may be any that keep to these rules, and one draw needn't show every extreme that they name: `signal`: values stay within the range, with cell-to-cell varying levels. `guard_cells`: some beam has exactly 8 guard cells. `train_cells`: the beam with 8 guard cells has 96 training cells. `offsets`: some beam has the offset 128 - 1.
All inputs are finite; a program needn't handle non-finite values.
Results may differ from the reference program's by a relative error of at most 0.001.
Values may be sent and summed in bfloat16 or wider, within the bound.
No kernel may reach another device: no remote copies, remote signals or barrier semaphores. Data moves between devices by JAX's collectives and lax.ppermute only.
A program may use at most 64 MiB of HBM per device.

```python
import jax
import jax.numpy as jnp
from jax import lax

TAPS = 2048
OFF_MAX = 128
GUARD_MAX = 8
TRAIN_MIN = 64
TRAIN_MAX = 96
BEAMS = 32
PULSES = 32
GATES = 4096


def chosen_beam(key):
    return jax.random.randint(jax.random.fold_in(key, 101), (), 0, BEAMS)


def draw_signal(key, part):
    shape = (BEAMS, PULSES, 2, GATES)
    base = jnp.clip(jax.random.normal(jax.random.fold_in(key, 11), shape, jnp.float32), -6.0, 6.0)
    levels = jnp.exp(jax.random.uniform(jax.random.fold_in(key, 12), (BEAMS, 1, 1, GATES), jnp.float32, -1.15, 1.15))
    values = base * levels
    return values.astype(jnp.bfloat16)


def draw_guard_cells(key, part):
    values = jax.random.randint(jax.random.fold_in(key, 1), (BEAMS,), 1, GUARD_MAX + 1)
    return values.at[chosen_beam(key)].set(GUARD_MAX).astype(jnp.int32)


def draw_train_cells(key, part):
    values = jax.random.randint(jax.random.fold_in(key, 2), (BEAMS,), TRAIN_MIN, TRAIN_MAX + 1)
    return values.at[chosen_beam(key)].set(TRAIN_MAX).astype(jnp.int32)


def draw_offsets(key, part):
    values = jax.random.randint(jax.random.fold_in(key, 3), (BEAMS,), 0, OFF_MAX)
    return values.at[chosen_beam(key)].set(OFF_MAX - 1).astype(jnp.int32)


def plant(entries, stream_key, low, top_value):
    longest = entries.shape.index(max(entries.shape))
    spots = []
    for shift in (0, 1):
        where = [jax.random.randint(jax.random.fold_in(stream_key, axis), (), 0, length) for axis, length in enumerate(entries.shape)]
        where[longest] = (where[longest] + shift) % entries.shape[longest]
        spots.append(tuple(where))
    return entries.at[spots[0]].set(low).at[spots[1]].set(top_value)


def shard_levels(key, shape, pieces, smallest, largest):
    loudness = 1.0
    for axis_at, shards_of in pieces:
        steps = jax.random.uniform(jax.random.fold_in(jax.random.fold_in(key, 6), axis_at), (shards_of,), jnp.float32, smallest / len(pieces), largest / len(pieces))
        loudness = loudness * jnp.repeat(jnp.exp(steps), shape[axis_at] // shards_of).reshape((-1,) + (1,) * (len(shape) - 1 - axis_at))
    return loudness


def scatter_about(key, extent, width, reach, shards=(), kind=jnp.bfloat16):
    entries = width * jax.random.normal(key, extent, jnp.float32)
    if shards:
        entries = entries * shard_levels(key, extent, shards, -0.22, 0.18)
    return jnp.clip(entries, -reach, reach).astype(kind)


def setup_inputs(seed: int = 0) -> dict:
    seeds = jax.random.split(jax.random.key(seed), 7)
    signal = draw_signal(jax.random.fold_in(seeds[6], 71), 0)
    replica = scatter_about(seeds[1], (2, TAPS), (2 * TAPS) ** -0.5, 0.09375, ((1, 64),))
    guard_cells = draw_guard_cells(jax.random.fold_in(seeds[6], 71), 0)
    train_cells = draw_train_cells(jax.random.fold_in(seeds[6], 71), 0)
    scale_index = plant(jax.random.randint(seeds[4], (BEAMS,), 0, 16), jax.random.fold_in(seeds[4], 1), 0, 15).astype(jnp.int32)
    offsets = draw_offsets(jax.random.fold_in(seeds[6], 71), 0)
    return {"signal": signal, "replica": replica, "guard_cells": guard_cells, "train_cells": train_cells, "scale_index": scale_index, "offsets": offsets}


EPSILON = 1e-6


def strip_ratio(power, guard, train, level, gates):
    margin = GUARD_MAX + TRAIN_MAX
    padded = jnp.pad(power, ((0, 0), (margin, margin)))
    prefix = jnp.concatenate([jnp.zeros((power.shape[0], 1), jnp.float32), jnp.cumsum(padded, axis=1)], axis=1)
    position = jnp.arange(gates, dtype=jnp.int32)
    centre = position + margin
    lag = jnp.take(prefix, centre - guard, axis=1) - jnp.take(prefix, centre - guard - train, axis=1)
    lead = jnp.take(prefix, centre + guard + train + 1, axis=1) - jnp.take(prefix, centre + guard + 1, axis=1)
    count = jnp.clip(position - guard, 0, train) + jnp.clip(gates - 1 - position - guard, 0, train)
    noise = (lag + lead) / count.astype(jnp.float32)[None, :]
    factor = jnp.exp2(level.astype(jnp.float32) / 8.0)
    return power / (factor * (noise + EPSILON))


def reference(signal, replica, guard_cells, train_cells, scale_index, offsets):
    gates = signal.shape[3]
    length = 1
    while length < gates + TAPS + OFF_MAX:
        length = length * 2
    taps_values = replica.astype(jnp.float32)
    kernel = jnp.conj(jnp.fft.fft(taps_values[0] + 1j * taps_values[1], length))

    def one(items):
        block, start, guard, train, level = items
        values = block.astype(jnp.float32)
        spectrum = jnp.fft.fft(values[:, 0] + 1j * values[:, 1], length, axis=-1)
        corr = jnp.fft.ifft(spectrum * kernel[None, :], axis=-1)
        window = lax.dynamic_slice_in_dim(corr, start.astype(jnp.int32), gates, 1)
        result = jnp.stack([jnp.real(window), jnp.imag(window)], axis=1).astype(jnp.float32).astype(jnp.bfloat16)
        real_part = result[:, 0].astype(jnp.float32)
        imag_part = result[:, 1].astype(jnp.float32)
        power = real_part * real_part + imag_part * imag_part
        return result, strip_ratio(power, guard, train, level, gates)

    compressed, test_ratio = lax.map(one, (signal, offsets, guard_cells, train_cells, scale_index))
    return compressed, test_ratio
```

```python
import functools

import jax
import jax.numpy as jnp
from jax import lax
from jax.experimental import pallas as pl
from jax.experimental.pallas import tpu as pltpu
from jax.sharding import PartitionSpec as P


TILE = 128
EPSILON = 1e-6
INNER = 4
TILES = INNER + 2
CHUNKS = 17
BLOCKS = TILES + CHUNKS - 1


def sent_to_all(array, axis):
    copies = jnp.broadcast_to(array, (lax.axis_size(axis), *array.shape))
    return lax.all_to_all(copies, axis, split_axis=0, concat_axis=0, tiled=True)


def passed_along(array, axis, by):
    devices = lax.axis_size(axis)
    pairs = [(i, i + by) for i in range(devices) if 0 <= i + by < devices]
    return lax.ppermute(array, axis, pairs)


def prepare(shards, place_ref, guard_ref, train_ref, scale_ref, offset_ref, *refs):
    pieces, outs = refs[:-6], refs[-6:]
    left_ref, right_ref, window_ref, slope_ref, floor_ref, edge_ref = outs
    place = place_ref[0]
    lane = lax.broadcasted_iota(jnp.int32, (8, TILE), 1)
    blocks = [(ref, at) for ref in pieces for at in range(0, ref.shape[3], TILE)]

    aligned = []
    for beam in range(2):
        offset = offset_ref[beam]
        shift = lax.rem(TILE - offset, TILE)
        whole = lane < TILE - offset
        parts = []
        for part in range(2):
            rolled = [
                pltpu.roll(ref[beam, part, :, at : at + TILE].astype(jnp.float32), shift, 1)
                for ref, at in blocks
            ]
            parts.append([jnp.where(whole, rolled[n], rolled[n + 1]) for n in range(BLOCKS)])
        aligned.append(parts)
    for n in range(BLOCKS):
        real = jnp.concatenate([aligned[0][0][n], aligned[1][0][n]], axis=0)
        imag = jnp.concatenate([aligned[0][1][n], aligned[1][1][n]], axis=0)
        at = 2 * n * TILE
        left_ref[:, at : at + TILE] = real.astype(jnp.bfloat16)
        left_ref[:, at + TILE : at + 2 * TILE] = imag.astype(jnp.bfloat16)
        right_ref[:, at : at + TILE] = imag.astype(jnp.bfloat16)
        right_ref[:, at + TILE : at + 2 * TILE] = (-real).astype(jnp.bfloat16)

    apart = jnp.abs(
        lax.broadcasted_iota(jnp.int32, (3 * TILE, TILE), 0)
        - TILE
        - lax.broadcasted_iota(jnp.int32, (3 * TILE, TILE), 1)
    )
    gate = place * (INNER * TILE) + lax.broadcasted_iota(jnp.int32, (8, INNER * TILE), 1)
    last = shards * INNER * TILE - 1
    for beam in range(2):
        guard = guard_ref[beam]
        train = train_ref[beam]
        inside = jnp.logical_and(apart > guard, apart <= guard + train)
        window_ref[:, beam * TILE : (beam + 1) * TILE] = jnp.where(inside, 1.0, 0.0).astype(
            jnp.bfloat16
        )
        count = jnp.clip(gate - guard, 0, train) + jnp.clip(last - gate - guard, 0, train)
        level = jnp.full((8, TILE), scale_ref[beam], jnp.int32).astype(jnp.float32)
        factor = jnp.exp2(level / 8.0)
        slope_ref[8 * beam : 8 * beam + 8, :] = jnp.concatenate(
            [factor] * INNER, axis=1
        ) / count.astype(jnp.float32)
        floor_ref[8 * beam : 8 * beam + 8, :] = factor * EPSILON
    edge_ref[0:8, :] = jnp.where(jnp.full((8, TILE), place, jnp.int32) > 0, 1.0, 0.0)
    edge_ref[8:16, :] = jnp.where(jnp.full((8, TILE), place, jnp.int32) < shards - 1, 1.0, 0.0)


def detect(taps_ref, left_ref, right_ref, window_ref, slope_ref, floor_ref, edge_ref, *outs):
    compressed_ref, ratio_ref = outs
    across = (((1,), (1,)), ((), ()))
    lane = lax.broadcasted_iota(jnp.int32, (8, TILE), 1)
    row = lax.broadcasted_iota(jnp.int32, (8, TILE), 0)

    rows = []
    for part in range(2):
        quarters = [taps_ref[pl.ds(2 * q + part, 16, stride=8), :] for q in range(4)]
        rows.append(jnp.concatenate(quarters, axis=1))

    total = jnp.zeros((2 * TILES * 16, TILE), jnp.float32)
    before = None
    for chunk in range(CHUNKS):
        rolled = []
        for part in range(2):
            if chunk < CHUNKS - 1:
                line = jnp.broadcast_to(rows[part][chunk : chunk + 1, :], (8, TILE))
                rolled.append(
                    [pltpu.roll(line, 8 * q, 1, stride=1, stride_axis=0) for q in range(16)]
                )
            else:
                rolled.append([jnp.zeros((8, TILE), jnp.float32)] * 16)
        panel = []
        for part in range(2):
            pieces = []
            for q in range(16):
                old = before[part][q] if before is not None else jnp.zeros((8, TILE), jnp.float32)
                pieces.append(jnp.where(lane >= 8 * q + row, rolled[part][q], old))
            panel.append(jnp.concatenate(pieces, axis=0).astype(jnp.bfloat16))
        before = rolled
        weights = jnp.concatenate(panel, axis=1)
        samples = [
            ref[:, 2 * (tile + chunk) * TILE : 2 * (tile + chunk + 1) * TILE]
            for ref in (left_ref, right_ref)
            for tile in range(TILES)
        ]
        total = total + lax.dot_general(
            jnp.concatenate(samples, axis=0), weights, across, preferred_element_type=jnp.float32
        )

    rounded = total.astype(jnp.bfloat16)
    half = TILES * 16
    power = []
    for tile in range(TILES):
        real = rounded[16 * tile : 16 * tile + 16]
        imag = rounded[half + 16 * tile : half + 16 * tile + 16]
        if 1 <= tile <= INNER:
            at = (tile - 1) * TILE
            for beam in range(2):
                compressed_ref[beam, 0, :, at : at + TILE] = real[8 * beam : 8 * beam + 8]
                compressed_ref[beam, 1, :, at : at + TILE] = imag[8 * beam : 8 * beam + 8]
        real = real.astype(jnp.float32)
        imag = imag.astype(jnp.float32)
        power.append(real * real + imag * imag)
    power[0] = power[0] * jnp.concatenate([edge_ref[0:8, :]] * 2, axis=0)
    power[-1] = power[-1] * jnp.concatenate([edge_ref[8:16, :]] * 2, axis=0)

    terms = []
    rest = power
    for _ in range(3):
        term = [cells.astype(jnp.bfloat16) for cells in rest]
        rest = [cells - t.astype(jnp.float32) for cells, t in zip(rest, term)]
        terms += [
            jnp.concatenate(term[tile - 1 : tile + 2], axis=1) for tile in range(1, INNER + 1)
        ]
    sums = lax.dot_general(
        jnp.concatenate(terms, axis=0),
        window_ref[...],
        (((1,), (0,)), ((), ())),
        preferred_element_type=jnp.float32,
    )
    size = INNER * 16
    sums = sums[2 * size :] + sums[size : 2 * size] + sums[:size]
    for tile in range(INNER):
        at = tile * TILE
        for beam in range(2):
            noise = sums[16 * tile + 8 * beam : 16 * tile + 8 * beam + 8]
            noise = noise[:, beam * TILE : (beam + 1) * TILE]
            rows_of = slice(8 * beam, 8 * beam + 8)
            ratio_ref[beam, :, at : at + TILE] = power[tile + 1][rows_of] / (
                noise * slope_ref[rows_of, at : at + TILE] + floor_ref[rows_of, :]
            )


def body(signal, replica, guard_cells, train_cells, scale_index, offsets):
    shards = lax.axis_size("range")
    vmem = pl.BlockSpec(memory_space=pltpu.VMEM)
    smem = pl.BlockSpec(memory_space=pltpu.SMEM)
    f32, bf16 = jnp.float32, jnp.bfloat16

    taps = sent_to_all(replica.astype(f32), ("beam", "pulse"))
    cells = jnp.transpose(signal, (0, 2, 1, 3))
    own = cells.shape[3]
    pieces = [passed_along(cells[..., own - TILE :], "range", 1), cells]
    pieces += [passed_along(cells, "range", -step) for step in range(1, 5)]
    pieces.append(passed_along(cells[..., : 2 * TILE], "range", -5))
    taps = taps.reshape(-1, taps.shape[-1])
    place = lax.axis_index("range").reshape(1)
    prepared = pl.pallas_call(
        functools.partial(prepare, shards),
        out_shape=(
            jax.ShapeDtypeStruct((16, 2 * BLOCKS * TILE), bf16),
            jax.ShapeDtypeStruct((16, 2 * BLOCKS * TILE), bf16),
            jax.ShapeDtypeStruct((3 * TILE, 2 * TILE), bf16),
            jax.ShapeDtypeStruct((16, INNER * TILE), f32),
            jax.ShapeDtypeStruct((16, TILE), f32),
            jax.ShapeDtypeStruct((16, TILE), f32),
        ),
        in_specs=[smem] * 5 + [vmem] * len(pieces),
        out_specs=[vmem] * 6,
        compiler_params=pltpu.CompilerParams(vmem_limit_bytes=4 << 20),
        cost_estimate=pl.CostEstimate(flops=1 << 20, bytes_accessed=1 << 20, transcendentals=0),
        name="prepare",
    )(place, guard_cells, train_cells, scale_index, offsets, *pieces)
    compressed, ratio = pl.pallas_call(
        detect,
        out_shape=(
            jax.ShapeDtypeStruct((2, 2, 8, INNER * TILE), bf16),
            jax.ShapeDtypeStruct((2, 8, INNER * TILE), f32),
        ),
        in_specs=[vmem] * 7,
        out_specs=[vmem] * 2,
        compiler_params=pltpu.CompilerParams(vmem_limit_bytes=4 << 20),
        cost_estimate=pl.CostEstimate(flops=1 << 28, bytes_accessed=1 << 20, transcendentals=0),
        name="detect",
    )(taps, *prepared)
    return jnp.transpose(compressed, (0, 2, 1, 3)), ratio


def solution(mesh):
    placed = (
        P("beam", "pulse", None, "range"),
        P(None, ("beam", "pulse")),
        P("beam"),
        P("beam"),
        P("beam"),
        P("beam"),
    )
    return jax.shard_map(
        body,
        mesh=mesh,
        in_specs=placed,
        out_specs=(P("beam", "pulse", None, "range"), P("beam", "pulse", "range")),
        check_vma=False,
    )
```

```python
import functools

import jax
import jax.numpy as jnp
from jax import lax
from jax.experimental import pallas as pl
from jax.experimental.pallas import tpu as pltpu
from jax.sharding import PartitionSpec as P


TILE = 128
EPSILON = 1e-6
INNER = 4
TILES = INNER + 2
CHUNKS = 17
BLOCKS = TILES + CHUNKS - 1


def sent_to_all(array, axis):
    copies = jnp.broadcast_to(array, (lax.axis_size(axis), *array.shape))
    return lax.all_to_all(copies, axis, split_axis=0, concat_axis=0, tiled=True)


def strip_of_chip(signal):
    devices = lax.axis_size("range")
    cells = jnp.transpose(signal, (0, 2, 1, 3))
    half = cells.shape[3] // 2
    own = jnp.stack([cells[..., :half], cells[..., half:]])

    def sent(array, pairs):
        inside = [(i, j) for i, j in pairs if 0 <= i < devices]
        return lax.ppermute(array, "range", inside)

    first = lax.rem(lax.axis_index("range"), 2) == 0
    ends = [(j + 6 if j % 2 == 0 else j - 2, j) for j in range(devices)]
    ahead = sent(own, [(j + 2, j) for j in range(devices)])
    farther = sent(own, [(j + 4, j) for j in range(devices)])
    rest = sent(jnp.where(first, own[:1], own[1:]), ends)
    mine = jnp.concatenate([own, ahead, farther, rest], axis=0)
    chips = [[2 * i, 2 * i + 1] for i in range(devices // 2)]
    return lax.all_gather(mine, "range", axis_index_groups=chips, tiled=True)


def prepare(shards, place_ref, guard_ref, train_ref, scale_ref, offset_ref, *refs):
    strip_ref, outs = refs[0], refs[1:]
    left_ref, right_ref, window_ref, slope_ref, floor_ref, edge_ref = outs
    place = place_ref[0]
    lane = lax.broadcasted_iota(jnp.int32, (8, TILE), 1)

    count = strip_ref.shape[0] // 2
    strip = [2 * count - 1]
    strip += [core * count + at + sub for at in (0, 2, 4) for core in (0, 1) for sub in (0, 1)]
    strip += [count - 1]
    core = lax.rem(place, 2)
    blocks = []
    for n in range(len(strip) - 2):
        piece = jnp.where(core == 0, strip[n], strip[n + 2])
        blocks += [(piece, at) for at in ((TILE,) if n == 0 else (0, TILE))]

    aligned = []
    for beam in range(2):
        offset = offset_ref[beam]
        shift = lax.rem(TILE - offset, TILE)
        whole = lane < TILE - offset
        parts = []
        for part in range(2):
            rolled = [
                pltpu.roll(
                    strip_ref[piece, beam, part, :, at : at + TILE].astype(jnp.float32), shift, 1
                )
                for piece, at in blocks
            ]
            parts.append([jnp.where(whole, rolled[n], rolled[n + 1]) for n in range(BLOCKS)])
        aligned.append(parts)
    for n in range(BLOCKS):
        real = jnp.concatenate([aligned[0][0][n], aligned[1][0][n]], axis=0)
        imag = jnp.concatenate([aligned[0][1][n], aligned[1][1][n]], axis=0)
        at = 2 * n * TILE
        left_ref[:, at : at + TILE] = real.astype(jnp.bfloat16)
        left_ref[:, at + TILE : at + 2 * TILE] = imag.astype(jnp.bfloat16)
        right_ref[:, at : at + TILE] = imag.astype(jnp.bfloat16)
        right_ref[:, at + TILE : at + 2 * TILE] = (-real).astype(jnp.bfloat16)

    apart = jnp.abs(
        lax.broadcasted_iota(jnp.int32, (3 * TILE, TILE), 0)
        - TILE
        - lax.broadcasted_iota(jnp.int32, (3 * TILE, TILE), 1)
    )
    gate = place * (INNER * TILE) + lax.broadcasted_iota(jnp.int32, (8, INNER * TILE), 1)
    last = shards * INNER * TILE - 1
    for beam in range(2):
        guard = guard_ref[beam]
        train = train_ref[beam]
        inside = jnp.logical_and(apart > guard, apart <= guard + train)
        window_ref[:, beam * TILE : (beam + 1) * TILE] = jnp.where(inside, 1.0, 0.0).astype(
            jnp.bfloat16
        )
        count = jnp.clip(gate - guard, 0, train) + jnp.clip(last - gate - guard, 0, train)
        level = jnp.full((8, TILE), scale_ref[beam], jnp.int32).astype(jnp.float32)
        factor = jnp.exp2(level / 8.0)
        slope_ref[8 * beam : 8 * beam + 8, :] = jnp.concatenate(
            [factor] * INNER, axis=1
        ) / count.astype(jnp.float32)
        floor_ref[8 * beam : 8 * beam + 8, :] = factor * EPSILON
    edge_ref[0:8, :] = jnp.where(jnp.full((8, TILE), place, jnp.int32) > 0, 1.0, 0.0)
    edge_ref[8:16, :] = jnp.where(jnp.full((8, TILE), place, jnp.int32) < shards - 1, 1.0, 0.0)


def detect(taps_ref, left_ref, right_ref, window_ref, slope_ref, floor_ref, edge_ref, *outs):
    compressed_ref, ratio_ref = outs
    across = (((1,), (1,)), ((), ()))
    lane = lax.broadcasted_iota(jnp.int32, (8, TILE), 1)
    row = lax.broadcasted_iota(jnp.int32, (8, TILE), 0)

    rows = []
    for part in range(2):
        quarters = [taps_ref[pl.ds(2 * q + part, 16, stride=8), :] for q in range(4)]
        rows.append(jnp.concatenate(quarters, axis=1))

    total = jnp.zeros((2 * TILES * 16, TILE), jnp.float32)
    before = None
    for chunk in range(CHUNKS):
        rolled = []
        for part in range(2):
            if chunk < CHUNKS - 1:
                line = jnp.broadcast_to(rows[part][chunk : chunk + 1, :], (8, TILE))
                rolled.append(
                    [pltpu.roll(line, 8 * q, 1, stride=1, stride_axis=0) for q in range(16)]
                )
            else:
                rolled.append([jnp.zeros((8, TILE), jnp.float32)] * 16)
        panel = []
        for part in range(2):
            pieces = []
            for q in range(16):
                old = before[part][q] if before is not None else jnp.zeros((8, TILE), jnp.float32)
                pieces.append(jnp.where(lane >= 8 * q + row, rolled[part][q], old))
            panel.append(jnp.concatenate(pieces, axis=0).astype(jnp.bfloat16))
        before = rolled
        weights = jnp.concatenate(panel, axis=1)
        samples = [
            ref[:, 2 * (tile + chunk) * TILE : 2 * (tile + chunk + 1) * TILE]
            for ref in (left_ref, right_ref)
            for tile in range(TILES)
        ]
        total = total + lax.dot_general(
            jnp.concatenate(samples, axis=0), weights, across, preferred_element_type=jnp.float32
        )

    rounded = total.astype(jnp.bfloat16)
    half = TILES * 16
    power = []
    for tile in range(TILES):
        real = rounded[16 * tile : 16 * tile + 16]
        imag = rounded[half + 16 * tile : half + 16 * tile + 16]
        if 1 <= tile <= INNER:
            at = (tile - 1) * TILE
            for beam in range(2):
                compressed_ref[beam, 0, :, at : at + TILE] = real[8 * beam : 8 * beam + 8]
                compressed_ref[beam, 1, :, at : at + TILE] = imag[8 * beam : 8 * beam + 8]
        real = real.astype(jnp.float32)
        imag = imag.astype(jnp.float32)
        power.append(real * real + imag * imag)
    power[0] = power[0] * jnp.concatenate([edge_ref[0:8, :]] * 2, axis=0)
    power[-1] = power[-1] * jnp.concatenate([edge_ref[8:16, :]] * 2, axis=0)

    terms = []
    rest = power
    for _ in range(3):
        term = [cells.astype(jnp.bfloat16) for cells in rest]
        rest = [cells - t.astype(jnp.float32) for cells, t in zip(rest, term)]
        terms += [
            jnp.concatenate(term[tile - 1 : tile + 2], axis=1) for tile in range(1, INNER + 1)
        ]
    sums = lax.dot_general(
        jnp.concatenate(terms, axis=0),
        window_ref[...],
        (((1,), (0,)), ((), ())),
        preferred_element_type=jnp.float32,
    )
    size = INNER * 16
    sums = sums[2 * size :] + sums[size : 2 * size] + sums[:size]
    for tile in range(INNER):
        at = tile * TILE
        for beam in range(2):
            noise = sums[16 * tile + 8 * beam : 16 * tile + 8 * beam + 8]
            noise = noise[:, beam * TILE : (beam + 1) * TILE]
            rows_of = slice(8 * beam, 8 * beam + 8)
            ratio_ref[beam, :, at : at + TILE] = power[tile + 1][rows_of] / (
                noise * slope_ref[rows_of, at : at + TILE] + floor_ref[rows_of, :]
            )


def body(signal, replica, guard_cells, train_cells, scale_index, offsets):
    shards = lax.axis_size("range")
    vmem = pl.BlockSpec(memory_space=pltpu.VMEM)
    smem = pl.BlockSpec(memory_space=pltpu.SMEM)
    f32, bf16 = jnp.float32, jnp.bfloat16

    taps = sent_to_all(replica.astype(f32), ("beam", "pulse"))
    strip = strip_of_chip(signal)
    taps = taps.reshape(-1, taps.shape[-1])
    place = lax.axis_index("range").reshape(1)
    prepared = pl.pallas_call(
        functools.partial(prepare, shards),
        out_shape=(
            jax.ShapeDtypeStruct((16, 2 * BLOCKS * TILE), bf16),
            jax.ShapeDtypeStruct((16, 2 * BLOCKS * TILE), bf16),
            jax.ShapeDtypeStruct((3 * TILE, 2 * TILE), bf16),
            jax.ShapeDtypeStruct((16, INNER * TILE), f32),
            jax.ShapeDtypeStruct((16, TILE), f32),
            jax.ShapeDtypeStruct((16, TILE), f32),
        ),
        in_specs=[smem] * 5 + [vmem],
        out_specs=[vmem] * 6,
        compiler_params=pltpu.CompilerParams(vmem_limit_bytes=4 << 20),
        cost_estimate=pl.CostEstimate(flops=1 << 20, bytes_accessed=1 << 20, transcendentals=0),
        name="prepare",
    )(place, guard_cells, train_cells, scale_index, offsets, strip)
    compressed, ratio = pl.pallas_call(
        detect,
        out_shape=(
            jax.ShapeDtypeStruct((2, 2, 8, INNER * TILE), bf16),
            jax.ShapeDtypeStruct((2, 8, INNER * TILE), f32),
        ),
        in_specs=[vmem] * 7,
        out_specs=[vmem] * 2,
        compiler_params=pltpu.CompilerParams(vmem_limit_bytes=4 << 20),
        cost_estimate=pl.CostEstimate(flops=1 << 28, bytes_accessed=1 << 20, transcendentals=0),
        name="detect",
    )(taps, *prepared)
    return jnp.transpose(compressed, (0, 2, 1, 3)), ratio


def solution(mesh):
    placed = (
        P("beam", "pulse", None, "range"),
        P(None, ("beam", "pulse")),
        P("beam"),
        P("beam"),
        P("beam"),
        P("beam"),
    )
    return jax.shard_map(
        body,
        mesh=mesh,
        in_specs=placed,
        out_specs=(P("beam", "pulse", None, "range"), P("beam", "pulse", "range")),
        check_vma=False,
    )
```

```python
import functools

import jax
import jax.numpy as jnp
from jax import lax
from jax.experimental import pallas as pl
from jax.experimental.pallas import tpu as pltpu
from jax.sharding import PartitionSpec as P


TILE = 128
EPSILON = 1e-6
INNER = 4
TILES = INNER + 2
CHUNKS = 17
BLOCKS = TILES + CHUNKS - 1


def sent_to_all(array, axis):
    copies = jnp.broadcast_to(array, (lax.axis_size(axis), *array.shape))
    return lax.all_to_all(copies, axis, split_axis=0, concat_axis=0, tiled=True)


def strip_of_chip(signal):
    devices = lax.axis_size("range")
    cells = jnp.transpose(signal, (0, 2, 1, 3))
    half = cells.shape[3] // 2
    own = jnp.stack([cells[..., :half], cells[..., half:]])

    def sent(array, pairs):
        inside = [(i, j) for i, j in pairs if 0 <= i < devices]
        return lax.ppermute(array, "range", inside)

    first = lax.rem(lax.axis_index("range"), 2) == 0
    ends = [(j + 6 if j % 2 == 0 else j - 2, j) for j in range(devices)]
    ahead = sent(own, [(j + 2, j) for j in range(devices)])
    farther = sent(own, [(j + 4, j) for j in range(devices)])
    rest = sent(jnp.where(first, own[:1], own[1:]), ends)
    mine = jnp.concatenate([own, ahead, farther, rest], axis=0)
    chips = [[2 * i, 2 * i + 1] for i in range(devices // 2)]
    return lax.all_gather(mine, "range", axis_index_groups=chips, tiled=True)


def tables(shards, place_ref, guard_ref, train_ref, scale_ref, offset_ref, *outs):
    window_ref, slope_ref, floor_ref, edge_ref, scalars_ref = outs
    place = place_ref[0]
    scalars_ref[0] = offset_ref[0]
    scalars_ref[1] = offset_ref[1]
    scalars_ref[2] = lax.rem(place, 2)
    apart = jnp.abs(
        lax.broadcasted_iota(jnp.int32, (3 * TILE, TILE), 0)
        - TILE
        - lax.broadcasted_iota(jnp.int32, (3 * TILE, TILE), 1)
    )
    gate = place * (INNER * TILE) + lax.broadcasted_iota(jnp.int32, (8, INNER * TILE), 1)
    last = shards * INNER * TILE - 1
    for beam in range(2):
        guard = guard_ref[beam]
        train = train_ref[beam]
        inside = jnp.logical_and(apart > guard, apart <= guard + train)
        window_ref[:, beam * TILE : (beam + 1) * TILE] = jnp.where(inside, 1.0, 0.0).astype(
            jnp.bfloat16
        )
        count = jnp.clip(gate - guard, 0, train) + jnp.clip(last - gate - guard, 0, train)
        level = jnp.full((8, TILE), scale_ref[beam], jnp.int32).astype(jnp.float32)
        factor = jnp.exp2(level / 8.0)
        slope_ref[8 * beam : 8 * beam + 8, :] = jnp.concatenate(
            [factor] * INNER, axis=1
        ) / count.astype(jnp.float32)
        floor_ref[8 * beam : 8 * beam + 8, :] = factor * EPSILON
    edge_ref[0:8, :] = jnp.where(jnp.full((8, TILE), place, jnp.int32) > 0, 1.0, 0.0)
    edge_ref[8:16, :] = jnp.where(jnp.full((8, TILE), place, jnp.int32) < shards - 1, 1.0, 0.0)


def prepare(scalars_ref, strip_ref, left_ref, right_ref):
    lane = lax.broadcasted_iota(jnp.int32, (8, TILE), 1)

    count = strip_ref.shape[0] // 2
    strip = [2 * count - 1]
    strip += [core * count + at + sub for at in (0, 2, 4) for core in (0, 1) for sub in (0, 1)]
    strip += [count - 1]
    core = scalars_ref[2]
    blocks = []
    for n in range(len(strip) - 2):
        piece = jnp.where(core == 0, strip[n], strip[n + 2])
        blocks += [(piece, at) for at in ((TILE,) if n == 0 else (0, TILE))]

    aligned = []
    for beam in range(2):
        offset = scalars_ref[beam]
        shift = lax.rem(TILE - offset, TILE)
        whole = lane < TILE - offset
        parts = []
        for part in range(2):
            rolled = [
                pltpu.roll(
                    strip_ref[piece, beam, part, :, at : at + TILE].astype(jnp.float32), shift, 1
                )
                for piece, at in blocks
            ]
            parts.append([jnp.where(whole, rolled[n], rolled[n + 1]) for n in range(BLOCKS)])
        aligned.append(parts)
    for n in range(BLOCKS):
        real = jnp.concatenate([aligned[0][0][n], aligned[1][0][n]], axis=0)
        imag = jnp.concatenate([aligned[0][1][n], aligned[1][1][n]], axis=0)
        at = 2 * n * TILE
        left_ref[:, at : at + TILE] = real.astype(jnp.bfloat16)
        left_ref[:, at + TILE : at + 2 * TILE] = imag.astype(jnp.bfloat16)
        right_ref[:, at : at + TILE] = imag.astype(jnp.bfloat16)
        right_ref[:, at + TILE : at + 2 * TILE] = (-real).astype(jnp.bfloat16)


def detect(taps_ref, left_ref, right_ref, window_ref, slope_ref, floor_ref, edge_ref, *outs):
    compressed_ref, ratio_ref = outs
    across = (((1,), (1,)), ((), ()))
    lane = lax.broadcasted_iota(jnp.int32, (8, TILE), 1)
    row = lax.broadcasted_iota(jnp.int32, (8, TILE), 0)

    rows = []
    for part in range(2):
        quarters = [taps_ref[pl.ds(2 * q + part, 16, stride=8), :] for q in range(4)]
        rows.append(jnp.concatenate(quarters, axis=1))

    total = jnp.zeros((2 * TILES * 16, TILE), jnp.float32)
    before = None
    for chunk in range(CHUNKS):
        rolled = []
        for part in range(2):
            if chunk < CHUNKS - 1:
                line = jnp.broadcast_to(rows[part][chunk : chunk + 1, :], (8, TILE))
                rolled.append(
                    [pltpu.roll(line, 8 * q, 1, stride=1, stride_axis=0) for q in range(16)]
                )
            else:
                rolled.append([jnp.zeros((8, TILE), jnp.float32)] * 16)
        panel = []
        for part in range(2):
            pieces = []
            for q in range(16):
                old = before[part][q] if before is not None else jnp.zeros((8, TILE), jnp.float32)
                pieces.append(jnp.where(lane >= 8 * q + row, rolled[part][q], old))
            panel.append(jnp.concatenate(pieces, axis=0).astype(jnp.bfloat16))
        before = rolled
        weights = jnp.concatenate(panel, axis=1)
        samples = [
            ref[:, 2 * (tile + chunk) * TILE : 2 * (tile + chunk + 1) * TILE]
            for ref in (left_ref, right_ref)
            for tile in range(TILES)
        ]
        total = total + lax.dot_general(
            jnp.concatenate(samples, axis=0), weights, across, preferred_element_type=jnp.float32
        )

    rounded = total.astype(jnp.bfloat16)
    half = TILES * 16
    power = []
    for tile in range(TILES):
        real = rounded[16 * tile : 16 * tile + 16]
        imag = rounded[half + 16 * tile : half + 16 * tile + 16]
        if 1 <= tile <= INNER:
            at = (tile - 1) * TILE
            for beam in range(2):
                compressed_ref[beam, 0, :, at : at + TILE] = real[8 * beam : 8 * beam + 8]
                compressed_ref[beam, 1, :, at : at + TILE] = imag[8 * beam : 8 * beam + 8]
        real = real.astype(jnp.float32)
        imag = imag.astype(jnp.float32)
        power.append(real * real + imag * imag)
    power[0] = power[0] * jnp.concatenate([edge_ref[0:8, :]] * 2, axis=0)
    power[-1] = power[-1] * jnp.concatenate([edge_ref[8:16, :]] * 2, axis=0)

    terms = []
    rest = power
    for _ in range(3):
        term = [cells.astype(jnp.bfloat16) for cells in rest]
        rest = [cells - t.astype(jnp.float32) for cells, t in zip(rest, term)]
        terms += [
            jnp.concatenate(term[tile - 1 : tile + 2], axis=1) for tile in range(1, INNER + 1)
        ]
    sums = lax.dot_general(
        jnp.concatenate(terms, axis=0),
        window_ref[...],
        (((1,), (0,)), ((), ())),
        preferred_element_type=jnp.float32,
    )
    size = INNER * 16
    sums = sums[2 * size :] + sums[size : 2 * size] + sums[:size]
    for tile in range(INNER):
        at = tile * TILE
        for beam in range(2):
            noise = sums[16 * tile + 8 * beam : 16 * tile + 8 * beam + 8]
            noise = noise[:, beam * TILE : (beam + 1) * TILE]
            rows_of = slice(8 * beam, 8 * beam + 8)
            ratio_ref[beam, :, at : at + TILE] = power[tile + 1][rows_of] / (
                noise * slope_ref[rows_of, at : at + TILE] + floor_ref[rows_of, :]
            )


def body(signal, replica, guard_cells, train_cells, scale_index, offsets):
    shards = lax.axis_size("range")
    vmem = pl.BlockSpec(memory_space=pltpu.VMEM)
    smem = pl.BlockSpec(memory_space=pltpu.SMEM)
    f32, bf16 = jnp.float32, jnp.bfloat16

    taps = sent_to_all(replica.astype(f32), ("beam", "pulse"))
    strip = strip_of_chip(signal)
    window, slope, floor, edge, scalars = pl.pallas_call(
        functools.partial(tables, shards),
        out_shape=(
            jax.ShapeDtypeStruct((3 * TILE, 2 * TILE), bf16),
            jax.ShapeDtypeStruct((16, INNER * TILE), f32),
            jax.ShapeDtypeStruct((16, TILE), f32),
            jax.ShapeDtypeStruct((16, TILE), f32),
            jax.ShapeDtypeStruct((3,), jnp.int32),
        ),
        in_specs=[smem] * 5,
        out_specs=[vmem] * 4 + [smem],
        compiler_params=pltpu.CompilerParams(vmem_limit_bytes=4 << 20),
        cost_estimate=pl.CostEstimate(flops=1 << 20, bytes_accessed=1 << 18, transcendentals=0),
        name="tables",
    )(lax.axis_index("range").reshape(1), guard_cells, train_cells, scale_index, offsets)
    taps = taps.reshape(-1, taps.shape[-1])
    left, right = pl.pallas_call(
        prepare,
        out_shape=[jax.ShapeDtypeStruct((16, 2 * BLOCKS * TILE), bf16)] * 2,
        in_specs=[smem, vmem],
        out_specs=[vmem] * 2,
        compiler_params=pltpu.CompilerParams(vmem_limit_bytes=4 << 20),
        cost_estimate=pl.CostEstimate(flops=1 << 20, bytes_accessed=1 << 20, transcendentals=0),
        name="prepare",
    )(scalars, strip)
    compressed, ratio = pl.pallas_call(
        detect,
        out_shape=(
            jax.ShapeDtypeStruct((2, 2, 8, INNER * TILE), bf16),
            jax.ShapeDtypeStruct((2, 8, INNER * TILE), f32),
        ),
        in_specs=[vmem] * 7,
        out_specs=[vmem] * 2,
        compiler_params=pltpu.CompilerParams(vmem_limit_bytes=4 << 20),
        cost_estimate=pl.CostEstimate(flops=1 << 28, bytes_accessed=1 << 20, transcendentals=0),
        name="detect",
    )(taps, left, right, window, slope, floor, edge)
    return jnp.transpose(compressed, (0, 2, 1, 3)), ratio


def solution(mesh):
    placed = (
        P("beam", "pulse", None, "range"),
        P(None, ("beam", "pulse")),
        P("beam"),
        P("beam"),
        P("beam"),
        P("beam"),
    )
    return jax.shard_map(
        body,
        mesh=mesh,
        in_specs=placed,
        out_specs=(P("beam", "pulse", None, "range"), P("beam", "pulse", "range")),
        check_vma=False,
    )
```

```python
import functools

import jax
import jax.numpy as jnp
from jax import lax
from jax.experimental import pallas as pl
from jax.experimental.pallas import tpu as pltpu
from jax.sharding import PartitionSpec as P


TILE = 128
EPSILON = 1e-6
INNER = 4
TILES = INNER + 2
CHUNKS = 17
BLOCKS = TILES + CHUNKS - 1


def sent_to_all(array, axis):
    copies = jnp.broadcast_to(array, (lax.axis_size(axis), *array.shape))
    return lax.all_to_all(copies, axis, split_axis=0, concat_axis=0, tiled=True)


def strip_of_chip(signal):
    devices = lax.axis_size("range")
    cells = jnp.transpose(signal, (0, 2, 1, 3))
    half = cells.shape[3] // 2
    own = jnp.stack([cells[..., :half], cells[..., half:]])

    def sent(array, pairs):
        inside = [(i, j) for i, j in pairs if 0 <= i < devices]
        return lax.ppermute(array, "range", inside)

    first = lax.rem(lax.axis_index("range"), 2) == 0
    ends = [(j + 6 if j % 2 == 0 else j - 2, j) for j in range(devices)]
    ahead = sent(own, [(j + 2, j) for j in range(devices)])
    farther = sent(own, [(j + 4, j) for j in range(devices)])
    rest = sent(jnp.where(first, own[:1], own[1:]), ends)
    mine = jnp.concatenate([own, ahead, farther, rest], axis=0)
    chips = [[2 * i, 2 * i + 1] for i in range(devices // 2)]
    return lax.all_gather(mine, "range", axis_index_groups=chips, tiled=True)


def tables(shards, place_ref, guard_ref, train_ref, scale_ref, offset_ref, *outs):
    window_ref, slope_ref, floor_ref, edge_ref, scalars_ref = outs
    place = place_ref[0]
    scalars_ref[0] = offset_ref[0]
    scalars_ref[1] = offset_ref[1]
    scalars_ref[2] = lax.rem(place, 2)
    apart = jnp.abs(
        lax.broadcasted_iota(jnp.int32, (3 * TILE, TILE), 0)
        - TILE
        - lax.broadcasted_iota(jnp.int32, (3 * TILE, TILE), 1)
    )
    gate = place * (INNER * TILE) + lax.broadcasted_iota(jnp.int32, (8, INNER * TILE), 1)
    last = shards * INNER * TILE - 1
    for beam in range(2):
        guard = guard_ref[beam]
        train = train_ref[beam]
        inside = jnp.logical_and(apart > guard, apart <= guard + train)
        window_ref[:, beam * TILE : (beam + 1) * TILE] = jnp.where(inside, 1.0, 0.0).astype(
            jnp.bfloat16
        )
        count = jnp.clip(gate - guard, 0, train) + jnp.clip(last - gate - guard, 0, train)
        level = jnp.full((8, TILE), scale_ref[beam], jnp.int32).astype(jnp.float32)
        factor = jnp.exp2(level / 8.0)
        slope_ref[8 * beam : 8 * beam + 8, :] = jnp.concatenate(
            [factor] * INNER, axis=1
        ) / count.astype(jnp.float32)
        floor_ref[8 * beam : 8 * beam + 8, :] = factor * EPSILON
    edge_ref[0:8, :] = jnp.where(jnp.full((8, TILE), place, jnp.int32) > 0, 1.0, 0.0)
    edge_ref[8:16, :] = jnp.where(jnp.full((8, TILE), place, jnp.int32) < shards - 1, 1.0, 0.0)


def prepare(scalars_ref, strip_ref, left_ref, right_ref):
    lane = lax.broadcasted_iota(jnp.int32, (8, TILE), 1)

    count = strip_ref.shape[0] // 2
    strip = [2 * count - 1]
    strip += [core * count + at + sub for at in (0, 2, 4) for core in (0, 1) for sub in (0, 1)]
    strip += [count - 1]
    core = scalars_ref[2]
    blocks = []
    for n in range(len(strip) - 2):
        piece = jnp.where(core == 0, strip[n], strip[n + 2])
        blocks += [(piece, at) for at in ((TILE,) if n == 0 else (0, TILE))]

    aligned = []
    for beam in range(2):
        offset = scalars_ref[beam]
        shift = lax.rem(TILE - offset, TILE)
        whole = lane < TILE - offset
        parts = []
        for part in range(2):
            rolled = [
                pltpu.roll(
                    strip_ref[piece, beam, part, :, at : at + TILE].astype(jnp.float32), shift, 1
                )
                for piece, at in blocks
            ]
            parts.append([jnp.where(whole, rolled[n], rolled[n + 1]) for n in range(BLOCKS)])
        aligned.append(parts)
    for n in range(BLOCKS):
        real = jnp.concatenate([aligned[0][0][n], aligned[1][0][n]], axis=0)
        imag = jnp.concatenate([aligned[0][1][n], aligned[1][1][n]], axis=0)
        at = 2 * n * TILE
        left_ref[:, at : at + TILE] = real.astype(jnp.bfloat16)
        left_ref[:, at + TILE : at + 2 * TILE] = imag.astype(jnp.bfloat16)
        right_ref[:, at : at + TILE] = imag.astype(jnp.bfloat16)
        right_ref[:, at + TILE : at + 2 * TILE] = (-real).astype(jnp.bfloat16)


def detect(taps_ref, left_ref, right_ref, window_ref, slope_ref, floor_ref, edge_ref, *outs):
    compressed_ref, ratio_ref, pairs_ref, lines_ref = outs
    across = (((1,), (1,)), ((), ()))
    lane = lax.broadcasted_iota(jnp.int32, (8, TILE), 1)
    row = lax.broadcasted_iota(jnp.int32, (8, TILE), 0)

    lines_ref[...] = taps_ref[...].astype(jnp.float32)
    rows = []
    for part in range(2):
        quarters = [lines_ref[pl.ds(2 * q + part, 16, stride=8), :] for q in range(4)]
        rows.append(jnp.concatenate(quarters, axis=1))

    total = jnp.zeros((2 * TILES * 16, TILE), jnp.float32)
    before = None
    for chunk in range(CHUNKS):
        rolled = []
        for part in range(2):
            if chunk < CHUNKS - 1:
                line = jnp.broadcast_to(rows[part][chunk : chunk + 1, :], (8, TILE))
                rolled.append(
                    [pltpu.roll(line, 8 * q, 1, stride=1, stride_axis=0) for q in range(16)]
                )
            else:
                rolled.append([jnp.zeros((8, TILE), jnp.float32)] * 16)
        panel = []
        for part in range(2):
            pieces = []
            for q in range(16):
                old = before[part][q] if before is not None else jnp.zeros((8, TILE), jnp.float32)
                pieces.append(jnp.where(lane >= 8 * q + row, rolled[part][q], old))
            panel.append(jnp.concatenate(pieces, axis=0).astype(jnp.bfloat16))
        before = rolled
        weights = jnp.concatenate(panel, axis=1)
        samples = [
            ref[:, 2 * (tile + chunk) * TILE : 2 * (tile + chunk + 1) * TILE]
            for ref in (left_ref, right_ref)
            for tile in range(TILES)
        ]
        total = total + lax.dot_general(
            jnp.concatenate(samples, axis=0), weights, across, preferred_element_type=jnp.float32
        )

    rounded = total.astype(jnp.bfloat16)
    half = TILES * 16
    power = []
    for tile in range(TILES):
        real = rounded[16 * tile : 16 * tile + 16]
        imag = rounded[half + 16 * tile : half + 16 * tile + 16]
        if 1 <= tile <= INNER:
            at = (tile - 1) * TILE
            for beam in range(2):
                rows_of = slice(8 * beam, 8 * beam + 8)
                spot = 2 * (tile - 1) + beam
                pairs_ref[spot, pl.ds(0, 8, stride=2), :] = real.astype(jnp.float32)[rows_of]
                pairs_ref[spot, pl.ds(1, 8, stride=2), :] = imag.astype(jnp.float32)[rows_of]
                pairs = pairs_ref[spot].astype(jnp.bfloat16)
                compressed_ref[beam, :, :, at : at + TILE] = pairs.reshape(8, 2, TILE)
        real = real.astype(jnp.float32)
        imag = imag.astype(jnp.float32)
        power.append(real * real + imag * imag)
    power[0] = power[0] * jnp.concatenate([edge_ref[0:8, :]] * 2, axis=0)
    power[-1] = power[-1] * jnp.concatenate([edge_ref[8:16, :]] * 2, axis=0)

    terms = []
    rest = power
    for _ in range(3):
        term = [cells.astype(jnp.bfloat16) for cells in rest]
        rest = [cells - t.astype(jnp.float32) for cells, t in zip(rest, term)]
        terms += [
            jnp.concatenate(term[tile - 1 : tile + 2], axis=1) for tile in range(1, INNER + 1)
        ]
    sums = lax.dot_general(
        jnp.concatenate(terms, axis=0),
        window_ref[...],
        (((1,), (0,)), ((), ())),
        preferred_element_type=jnp.float32,
    )
    size = INNER * 16
    sums = sums[2 * size :] + sums[size : 2 * size] + sums[:size]
    for tile in range(INNER):
        at = tile * TILE
        for beam in range(2):
            noise = sums[16 * tile + 8 * beam : 16 * tile + 8 * beam + 8]
            noise = noise[:, beam * TILE : (beam + 1) * TILE]
            rows_of = slice(8 * beam, 8 * beam + 8)
            ratio_ref[beam, :, at : at + TILE] = power[tile + 1][rows_of] / (
                noise * slope_ref[rows_of, at : at + TILE] + floor_ref[rows_of, :]
            )


def body(signal, replica, guard_cells, train_cells, scale_index, offsets):
    shards = lax.axis_size("range")
    vmem = pl.BlockSpec(memory_space=pltpu.VMEM)
    smem = pl.BlockSpec(memory_space=pltpu.SMEM)
    f32, bf16 = jnp.float32, jnp.bfloat16

    taps = sent_to_all(replica, ("beam", "pulse"))
    strip = strip_of_chip(signal)
    window, slope, floor, edge, scalars = pl.pallas_call(
        functools.partial(tables, shards),
        out_shape=(
            jax.ShapeDtypeStruct((3 * TILE, 2 * TILE), bf16),
            jax.ShapeDtypeStruct((16, INNER * TILE), f32),
            jax.ShapeDtypeStruct((16, TILE), f32),
            jax.ShapeDtypeStruct((16, TILE), f32),
            jax.ShapeDtypeStruct((3,), jnp.int32),
        ),
        in_specs=[smem] * 5,
        out_specs=[vmem] * 4 + [smem],
        compiler_params=pltpu.CompilerParams(vmem_limit_bytes=4 << 20),
        cost_estimate=pl.CostEstimate(flops=1 << 20, bytes_accessed=1 << 18, transcendentals=0),
        name="tables",
    )(lax.axis_index("range").reshape(1), guard_cells, train_cells, scale_index, offsets)
    taps = taps.reshape(-1, taps.shape[-1])
    left, right = pl.pallas_call(
        prepare,
        out_shape=[jax.ShapeDtypeStruct((16, 2 * BLOCKS * TILE), bf16)] * 2,
        in_specs=[smem, vmem],
        out_specs=[vmem] * 2,
        compiler_params=pltpu.CompilerParams(vmem_limit_bytes=4 << 20),
        cost_estimate=pl.CostEstimate(flops=1 << 20, bytes_accessed=1 << 20, transcendentals=0),
        name="prepare",
    )(scalars, strip)
    compressed, ratio = pl.pallas_call(
        detect,
        out_shape=(
            jax.ShapeDtypeStruct((2, 8, 2, INNER * TILE), bf16),
            jax.ShapeDtypeStruct((2, 8, INNER * TILE), f32),
        ),
        in_specs=[vmem] * 7,
        out_specs=[vmem] * 2,
        scratch_shapes=[pltpu.VMEM((2 * INNER, 16, TILE), f32), pltpu.VMEM(taps.shape, f32)],
        compiler_params=pltpu.CompilerParams(vmem_limit_bytes=4 << 20),
        cost_estimate=pl.CostEstimate(flops=1 << 28, bytes_accessed=1 << 20, transcendentals=0),
        name="detect",
    )(taps, left, right, window, slope, floor, edge)
    return compressed, ratio


def solution(mesh):
    placed = (
        P("beam", "pulse", None, "range"),
        P(None, ("beam", "pulse")),
        P("beam"),
        P("beam"),
        P("beam"),
        P("beam"),
    )
    return jax.shard_map(
        body,
        mesh=mesh,
        in_specs=placed,
        out_specs=(P("beam", "pulse", None, "range"), P("beam", "pulse", "range")),
        check_vma=False,
    )
```

```python
import functools

import jax
import jax.numpy as jnp
from jax import lax
from jax.experimental import pallas as pl
from jax.experimental.pallas import tpu as pltpu
from jax.sharding import PartitionSpec as P


TILE = 128
EPSILON = 1e-6
INNER = 4
TILES = INNER + 2
CHUNKS = 17
BLOCKS = TILES + CHUNKS - 1


FIRST = 12


def sent_to_all(array, axes):
    beams, pulses = (lax.axis_size(axis) for axis in axes)
    order = [((FIRST + i) % beams) * pulses + j for i in range(beams) for j in range(pulses)]
    copies = jnp.broadcast_to(array, (beams * pulses, *array.shape))
    return lax.all_to_all(
        copies, axes, split_axis=0, concat_axis=0, tiled=True, axis_index_groups=[order]
    )


def strip_of_chip(signal):
    devices = lax.axis_size("range")
    cells = jnp.transpose(signal, (0, 2, 1, 3))
    half = cells.shape[3] // 2
    own = jnp.stack([cells[..., :half], cells[..., half:]])

    def sent(array, pairs):
        inside = [(i, j) for i, j in pairs if 0 <= i < devices]
        return lax.ppermute(array, "range", inside)

    first = lax.rem(lax.axis_index("range"), 2) == 0
    ends = [(j + 6 if j % 2 == 0 else j - 2, j) for j in range(devices)]
    ahead = sent(own, [(j + 2, j) for j in range(devices)])
    farther = sent(own, [(j + 4, j) for j in range(devices)])
    rest = sent(jnp.where(first, own[:1], own[1:]), ends)
    mine = jnp.concatenate([own, ahead, farther, rest], axis=0)
    chips = [[2 * i, 2 * i + 1] for i in range(devices // 2)]
    return lax.all_gather(mine, "range", axis_index_groups=chips, tiled=True)


def tables(shards, place_ref, guard_ref, train_ref, scale_ref, offset_ref, *outs):
    window_ref, slope_ref, floor_ref, edge_ref, scalars_ref = outs
    place = place_ref[0]
    scalars_ref[0] = offset_ref[0]
    scalars_ref[1] = offset_ref[1]
    scalars_ref[2] = lax.rem(place, 2)
    apart = jnp.abs(
        lax.broadcasted_iota(jnp.int32, (3 * TILE, TILE), 0)
        - TILE
        - lax.broadcasted_iota(jnp.int32, (3 * TILE, TILE), 1)
    )
    gate = place * (INNER * TILE) + lax.broadcasted_iota(jnp.int32, (8, INNER * TILE), 1)
    last = shards * INNER * TILE - 1
    for beam in range(2):
        guard = guard_ref[beam]
        train = train_ref[beam]
        inside = jnp.logical_and(apart > guard, apart <= guard + train)
        window_ref[:, beam * TILE : (beam + 1) * TILE] = jnp.where(inside, 1.0, 0.0).astype(
            jnp.bfloat16
        )
        count = jnp.clip(gate - guard, 0, train) + jnp.clip(last - gate - guard, 0, train)
        level = jnp.full((8, TILE), scale_ref[beam], jnp.int32).astype(jnp.float32)
        factor = jnp.exp2(level / 8.0)
        slope_ref[8 * beam : 8 * beam + 8, :] = jnp.concatenate(
            [factor] * INNER, axis=1
        ) / count.astype(jnp.float32)
        floor_ref[8 * beam : 8 * beam + 8, :] = factor * EPSILON
    edge_ref[0:8, :] = jnp.where(jnp.full((8, TILE), place, jnp.int32) > 0, 1.0, 0.0)
    edge_ref[8:16, :] = jnp.where(jnp.full((8, TILE), place, jnp.int32) < shards - 1, 1.0, 0.0)


def prepare(scalars_ref, strip_ref, left_ref, right_ref):
    lane = lax.broadcasted_iota(jnp.int32, (8, TILE), 1)

    count = strip_ref.shape[0] // 2
    strip = [2 * count - 1]
    strip += [core * count + at + sub for at in (0, 2, 4) for core in (0, 1) for sub in (0, 1)]
    strip += [count - 1]
    core = scalars_ref[2]
    blocks = []
    for n in range(len(strip) - 2):
        piece = jnp.where(core == 0, strip[n], strip[n + 2])
        blocks += [(piece, at) for at in ((TILE,) if n == 0 else (0, TILE))]

    aligned = []
    for beam in range(2):
        offset = scalars_ref[beam]
        shift = lax.rem(TILE - offset, TILE)
        whole = lane < TILE - offset
        parts = []
        for part in range(2):
            rolled = [
                pltpu.roll(
                    strip_ref[piece, beam, part, :, at : at + TILE].astype(jnp.float32), shift, 1
                )
                for piece, at in blocks
            ]
            parts.append([jnp.where(whole, rolled[n], rolled[n + 1]) for n in range(BLOCKS)])
        aligned.append(parts)
    for n in range(BLOCKS):
        real = jnp.concatenate([aligned[0][0][n], aligned[1][0][n]], axis=0)
        imag = jnp.concatenate([aligned[0][1][n], aligned[1][1][n]], axis=0)
        at = 2 * n * TILE
        left_ref[:, at : at + TILE] = real.astype(jnp.bfloat16)
        left_ref[:, at + TILE : at + 2 * TILE] = imag.astype(jnp.bfloat16)
        right_ref[:, at : at + TILE] = imag.astype(jnp.bfloat16)
        right_ref[:, at + TILE : at + 2 * TILE] = (-real).astype(jnp.bfloat16)


def detect(taps_ref, left_ref, right_ref, window_ref, slope_ref, floor_ref, edge_ref, *outs):
    compressed_ref, ratio_ref, pairs_ref, lines_ref = outs
    across = (((1,), (1,)), ((), ()))
    lane = lax.broadcasted_iota(jnp.int32, (8, TILE), 1)
    row = lax.broadcasted_iota(jnp.int32, (8, TILE), 0)

    lines_ref[...] = taps_ref[...].astype(jnp.float32)
    rows = []
    for part in range(2):
        quarters = [lines_ref[pl.ds(2 * q + part, 16, stride=8), :] for q in range(4)]
        rows.append(jnp.concatenate(quarters, axis=1))

    total = jnp.zeros((2 * TILES * 16, TILE), jnp.float32)
    before = None
    for chunk in range(CHUNKS):
        rolled = []
        for part in range(2):
            if chunk < CHUNKS - 1:
                at = (chunk - FIRST) % (CHUNKS - 1)
                line = jnp.broadcast_to(rows[part][at : at + 1, :], (8, TILE))
                rolled.append(
                    [pltpu.roll(line, 8 * q, 1, stride=1, stride_axis=0) for q in range(16)]
                )
            else:
                rolled.append([jnp.zeros((8, TILE), jnp.float32)] * 16)
        panel = []
        for part in range(2):
            pieces = []
            for q in range(16):
                old = before[part][q] if before is not None else jnp.zeros((8, TILE), jnp.float32)
                pieces.append(jnp.where(lane >= 8 * q + row, rolled[part][q], old))
            panel.append(jnp.concatenate(pieces, axis=0).astype(jnp.bfloat16))
        before = rolled
        weights = jnp.concatenate(panel, axis=1)
        samples = [
            ref[:, 2 * (tile + chunk) * TILE : 2 * (tile + chunk + 1) * TILE]
            for ref in (left_ref, right_ref)
            for tile in range(TILES)
        ]
        total = total + lax.dot_general(
            jnp.concatenate(samples, axis=0), weights, across, preferred_element_type=jnp.float32
        )

    rounded = total.astype(jnp.bfloat16)
    half = TILES * 16
    power = []
    for tile in range(TILES):
        real = rounded[16 * tile : 16 * tile + 16]
        imag = rounded[half + 16 * tile : half + 16 * tile + 16]
        if 1 <= tile <= INNER:
            at = (tile - 1) * TILE
            for beam in range(2):
                rows_of = slice(8 * beam, 8 * beam + 8)
                spot = 2 * (tile - 1) + beam
                pairs_ref[spot, pl.ds(0, 8, stride=2), :] = real.astype(jnp.float32)[rows_of]
                pairs_ref[spot, pl.ds(1, 8, stride=2), :] = imag.astype(jnp.float32)[rows_of]
                pairs = pairs_ref[spot].astype(jnp.bfloat16)
                compressed_ref[beam, :, :, at : at + TILE] = pairs.reshape(8, 2, TILE)
        real = real.astype(jnp.float32)
        imag = imag.astype(jnp.float32)
        power.append(real * real + imag * imag)
    power[0] = power[0] * jnp.concatenate([edge_ref[0:8, :]] * 2, axis=0)
    power[-1] = power[-1] * jnp.concatenate([edge_ref[8:16, :]] * 2, axis=0)

    terms = []
    rest = power
    for _ in range(3):
        term = [cells.astype(jnp.bfloat16) for cells in rest]
        rest = [cells - t.astype(jnp.float32) for cells, t in zip(rest, term)]
        terms += [
            jnp.concatenate(term[tile - 1 : tile + 2], axis=1) for tile in range(1, INNER + 1)
        ]
    sums = lax.dot_general(
        jnp.concatenate(terms, axis=0),
        window_ref[...],
        (((1,), (0,)), ((), ())),
        preferred_element_type=jnp.float32,
    )
    size = INNER * 16
    sums = sums[2 * size :] + sums[size : 2 * size] + sums[:size]
    for tile in range(INNER):
        at = tile * TILE
        for beam in range(2):
            noise = sums[16 * tile + 8 * beam : 16 * tile + 8 * beam + 8]
            noise = noise[:, beam * TILE : (beam + 1) * TILE]
            rows_of = slice(8 * beam, 8 * beam + 8)
            ratio_ref[beam, :, at : at + TILE] = power[tile + 1][rows_of] / (
                noise * slope_ref[rows_of, at : at + TILE] + floor_ref[rows_of, :]
            )


def body(signal, replica, guard_cells, train_cells, scale_index, offsets):
    shards = lax.axis_size("range")
    vmem = pl.BlockSpec(memory_space=pltpu.VMEM)
    smem = pl.BlockSpec(memory_space=pltpu.SMEM)
    f32, bf16 = jnp.float32, jnp.bfloat16

    taps = sent_to_all(replica, ("beam", "pulse"))
    strip = strip_of_chip(signal)
    window, slope, floor, edge, scalars = pl.pallas_call(
        functools.partial(tables, shards),
        out_shape=(
            jax.ShapeDtypeStruct((3 * TILE, 2 * TILE), bf16),
            jax.ShapeDtypeStruct((16, INNER * TILE), f32),
            jax.ShapeDtypeStruct((16, TILE), f32),
            jax.ShapeDtypeStruct((16, TILE), f32),
            jax.ShapeDtypeStruct((3,), jnp.int32),
        ),
        in_specs=[smem] * 5,
        out_specs=[vmem] * 4 + [smem],
        compiler_params=pltpu.CompilerParams(vmem_limit_bytes=4 << 20),
        cost_estimate=pl.CostEstimate(flops=1 << 20, bytes_accessed=1 << 18, transcendentals=0),
        name="tables",
    )(lax.axis_index("range").reshape(1), guard_cells, train_cells, scale_index, offsets)
    taps = taps.reshape(-1, taps.shape[-1])
    left, right = pl.pallas_call(
        prepare,
        out_shape=[jax.ShapeDtypeStruct((16, 2 * BLOCKS * TILE), bf16)] * 2,
        in_specs=[smem, vmem],
        out_specs=[vmem] * 2,
        compiler_params=pltpu.CompilerParams(vmem_limit_bytes=4 << 20),
        cost_estimate=pl.CostEstimate(flops=1 << 20, bytes_accessed=1 << 20, transcendentals=0),
        name="prepare",
    )(scalars, strip)
    compressed, ratio = pl.pallas_call(
        detect,
        out_shape=(
            jax.ShapeDtypeStruct((2, 8, 2, INNER * TILE), bf16),
            jax.ShapeDtypeStruct((2, 8, INNER * TILE), f32),
        ),
        in_specs=[vmem] * 7,
        out_specs=[vmem] * 2,
        scratch_shapes=[pltpu.VMEM((2 * INNER, 16, TILE), f32), pltpu.VMEM(taps.shape, f32)],
        compiler_params=pltpu.CompilerParams(vmem_limit_bytes=4 << 20),
        cost_estimate=pl.CostEstimate(flops=1 << 28, bytes_accessed=1 << 20, transcendentals=0),
        name="detect",
    )(taps, left, right, window, slope, floor, edge)
    return compressed, ratio


def solution(mesh):
    placed = (
        P("beam", "pulse", None, "range"),
        P(None, ("beam", "pulse")),
        P("beam"),
        P("beam"),
        P("beam"),
        P("beam"),
    )
    return jax.shard_map(
        body,
        mesh=mesh,
        in_specs=placed,
        out_specs=(P("beam", "pulse", None, "range"), P("beam", "pulse", "range")),
        check_vma=False,
    )
```

```python
import functools

import jax
import jax.numpy as jnp
from jax import lax
from jax.experimental import pallas as pl
from jax.experimental.pallas import tpu as pltpu
from jax.sharding import PartitionSpec as P


TILE = 128
EPSILON = 1e-6
INNER = 4
TILES = INNER + 2
CHUNKS = 17
BLOCKS = TILES + CHUNKS - 1


EARLY = 6
FIRST = 12


def sent_to_all(array, axes):
    beams, pulses = (lax.axis_size(axis) for axis in axes)
    order = [((FIRST + i) % beams) * pulses + j for i in range(beams) for j in range(pulses)]
    copies = jnp.broadcast_to(array, (beams * pulses, *array.shape))
    return lax.all_to_all(
        copies, axes, split_axis=0, concat_axis=0, tiled=True, axis_index_groups=[order]
    )


def strip_of_chip(signal):
    devices = lax.axis_size("range")
    cells = jnp.transpose(signal, (0, 2, 1, 3))
    half = cells.shape[3] // 2
    own = jnp.stack([cells[..., :half], cells[..., half:]])

    first = lax.rem(lax.axis_index("range"), 2) == 0
    ends = [(j + 6 if j % 2 == 0 else j - 2, j) for j in range(devices)]
    second = [(j + 4, j) for j in range(devices)]
    near = [(j + 2, j) for j in range(devices)]
    planes = lax.axis_size("beam")
    early = lax.axis_index("beam") < EARLY

    def sent(array, early_pairs, late_pairs):
        pairs = [(b * devices + i, b * devices + j) for b in range(EARLY) for i, j in early_pairs]
        pairs += [(b * devices + i, b * devices + j) for b in range(EARLY, planes) for i, j in late_pairs]
        inside = [(i, j) for i, j in pairs if i // devices == j // devices and i >= 0]
        return lax.ppermute(array, ("beam", "range"), inside)

    edge = jnp.where(first, own[:1], own[1:])
    got0 = sent(edge, ends, [])
    got1 = sent(jnp.where(early, own, jnp.concatenate([edge, edge])), second, ends)
    got2 = sent(own, near, second)
    got3 = sent(own, [], near)
    ahead = jnp.where(early, got2, got3)
    farther = jnp.where(early, got1, got2)
    rest = jnp.where(early, got0, got1[:1])
    mine = jnp.concatenate([own, ahead, farther, rest], axis=0)
    chips = [[2 * i, 2 * i + 1] for i in range(devices // 2)]
    return lax.all_gather(mine, "range", axis_index_groups=chips, tiled=True)


def tables(shards, place_ref, guard_ref, train_ref, scale_ref, offset_ref, *outs):
    window_ref, slope_ref, floor_ref, edge_ref, scalars_ref = outs
    place = place_ref[0]
    scalars_ref[0] = offset_ref[0]
    scalars_ref[1] = offset_ref[1]
    scalars_ref[2] = lax.rem(place, 2)
    apart = jnp.abs(
        lax.broadcasted_iota(jnp.int32, (3 * TILE, TILE), 0)
        - TILE
        - lax.broadcasted_iota(jnp.int32, (3 * TILE, TILE), 1)
    )
    gate = place * (INNER * TILE) + lax.broadcasted_iota(jnp.int32, (8, INNER * TILE), 1)
    last = shards * INNER * TILE - 1
    for beam in range(2):
        guard = guard_ref[beam]
        train = train_ref[beam]
        inside = jnp.logical_and(apart > guard, apart <= guard + train)
        window_ref[:, beam * TILE : (beam + 1) * TILE] = jnp.where(inside, 1.0, 0.0).astype(
            jnp.bfloat16
        )
        count = jnp.clip(gate - guard, 0, train) + jnp.clip(last - gate - guard, 0, train)
        level = jnp.full((8, TILE), scale_ref[beam], jnp.int32).astype(jnp.float32)
        factor = jnp.exp2(level / 8.0)
        slope_ref[8 * beam : 8 * beam + 8, :] = jnp.concatenate(
            [factor] * INNER, axis=1
        ) / count.astype(jnp.float32)
        floor_ref[8 * beam : 8 * beam + 8, :] = factor * EPSILON
    edge_ref[0:8, :] = jnp.where(jnp.full((8, TILE), place, jnp.int32) > 0, 1.0, 0.0)
    edge_ref[8:16, :] = jnp.where(jnp.full((8, TILE), place, jnp.int32) < shards - 1, 1.0, 0.0)


def prepare(scalars_ref, strip_ref, left_ref, right_ref):
    lane = lax.broadcasted_iota(jnp.int32, (8, TILE), 1)

    count = strip_ref.shape[0] // 2
    strip = [2 * count - 1]
    strip += [core * count + at + sub for at in (0, 2, 4) for core in (0, 1) for sub in (0, 1)]
    strip += [count - 1]
    core = scalars_ref[2]
    blocks = []
    for n in range(len(strip) - 2):
        piece = jnp.where(core == 0, strip[n], strip[n + 2])
        blocks += [(piece, at) for at in ((TILE,) if n == 0 else (0, TILE))]

    aligned = []
    for beam in range(2):
        offset = scalars_ref[beam]
        shift = lax.rem(TILE - offset, TILE)
        whole = lane < TILE - offset
        parts = []
        for part in range(2):
            rolled = [
                pltpu.roll(
                    strip_ref[piece, beam, part, :, at : at + TILE].astype(jnp.float32), shift, 1
                )
                for piece, at in blocks
            ]
            parts.append([jnp.where(whole, rolled[n], rolled[n + 1]) for n in range(BLOCKS)])
        aligned.append(parts)
    for n in range(BLOCKS):
        real = jnp.concatenate([aligned[0][0][n], aligned[1][0][n]], axis=0)
        imag = jnp.concatenate([aligned[0][1][n], aligned[1][1][n]], axis=0)
        at = 2 * n * TILE
        left_ref[:, at : at + TILE] = real.astype(jnp.bfloat16)
        left_ref[:, at + TILE : at + 2 * TILE] = imag.astype(jnp.bfloat16)
        right_ref[:, at : at + TILE] = imag.astype(jnp.bfloat16)
        right_ref[:, at + TILE : at + 2 * TILE] = (-real).astype(jnp.bfloat16)


def detect(taps_ref, left_ref, right_ref, window_ref, slope_ref, floor_ref, edge_ref, *outs):
    compressed_ref, ratio_ref, pairs_ref, lines_ref = outs
    across = (((1,), (1,)), ((), ()))
    lane = lax.broadcasted_iota(jnp.int32, (8, TILE), 1)
    row = lax.broadcasted_iota(jnp.int32, (8, TILE), 0)

    lines_ref[...] = taps_ref[...].astype(jnp.float32)
    rows = []
    for part in range(2):
        quarters = [lines_ref[pl.ds(2 * q + part, 16, stride=8), :] for q in range(4)]
        rows.append(jnp.concatenate(quarters, axis=1))

    total = jnp.zeros((2 * TILES * 16, TILE), jnp.float32)
    before = None
    for chunk in range(CHUNKS):
        rolled = []
        for part in range(2):
            if chunk < CHUNKS - 1:
                at = (chunk - FIRST) % (CHUNKS - 1)
                line = jnp.broadcast_to(rows[part][at : at + 1, :], (8, TILE))
                rolled.append(
                    [pltpu.roll(line, 8 * q, 1, stride=1, stride_axis=0) for q in range(16)]
                )
            else:
                rolled.append([jnp.zeros((8, TILE), jnp.float32)] * 16)
        panel = []
        for part in range(2):
            pieces = []
            for q in range(16):
                old = before[part][q] if before is not None else jnp.zeros((8, TILE), jnp.float32)
                pieces.append(jnp.where(lane >= 8 * q + row, rolled[part][q], old))
            panel.append(jnp.concatenate(pieces, axis=0).astype(jnp.bfloat16))
        before = rolled
        weights = jnp.concatenate(panel, axis=1)
        samples = [
            ref[:, 2 * (tile + chunk) * TILE : 2 * (tile + chunk + 1) * TILE]
            for ref in (left_ref, right_ref)
            for tile in range(TILES)
        ]
        total = total + lax.dot_general(
            jnp.concatenate(samples, axis=0), weights, across, preferred_element_type=jnp.float32
        )

    rounded = total.astype(jnp.bfloat16)
    half = TILES * 16
    power = []
    for tile in range(TILES):
        real = rounded[16 * tile : 16 * tile + 16]
        imag = rounded[half + 16 * tile : half + 16 * tile + 16]
        if 1 <= tile <= INNER:
            at = (tile - 1) * TILE
            for beam in range(2):
                rows_of = slice(8 * beam, 8 * beam + 8)
                spot = 2 * (tile - 1) + beam
                pairs_ref[spot, pl.ds(0, 8, stride=2), :] = real.astype(jnp.float32)[rows_of]
                pairs_ref[spot, pl.ds(1, 8, stride=2), :] = imag.astype(jnp.float32)[rows_of]
                pairs = pairs_ref[spot].astype(jnp.bfloat16)
                compressed_ref[beam, :, :, at : at + TILE] = pairs.reshape(8, 2, TILE)
        real = real.astype(jnp.float32)
        imag = imag.astype(jnp.float32)
        power.append(real * real + imag * imag)
    power[0] = power[0] * jnp.concatenate([edge_ref[0:8, :]] * 2, axis=0)
    power[-1] = power[-1] * jnp.concatenate([edge_ref[8:16, :]] * 2, axis=0)

    terms = []
    rest = power
    for _ in range(3):
        term = [cells.astype(jnp.bfloat16) for cells in rest]
        rest = [cells - t.astype(jnp.float32) for cells, t in zip(rest, term)]
        terms += [
            jnp.concatenate(term[tile - 1 : tile + 2], axis=1) for tile in range(1, INNER + 1)
        ]
    sums = lax.dot_general(
        jnp.concatenate(terms, axis=0),
        window_ref[...],
        (((1,), (0,)), ((), ())),
        preferred_element_type=jnp.float32,
    )
    size = INNER * 16
    sums = sums[2 * size :] + sums[size : 2 * size] + sums[:size]
    for tile in range(INNER):
        at = tile * TILE
        for beam in range(2):
            noise = sums[16 * tile + 8 * beam : 16 * tile + 8 * beam + 8]
            noise = noise[:, beam * TILE : (beam + 1) * TILE]
            rows_of = slice(8 * beam, 8 * beam + 8)
            ratio_ref[beam, :, at : at + TILE] = power[tile + 1][rows_of] / (
                noise * slope_ref[rows_of, at : at + TILE] + floor_ref[rows_of, :]
            )


def body(signal, replica, guard_cells, train_cells, scale_index, offsets):
    shards = lax.axis_size("range")
    vmem = pl.BlockSpec(memory_space=pltpu.VMEM)
    smem = pl.BlockSpec(memory_space=pltpu.SMEM)
    f32, bf16 = jnp.float32, jnp.bfloat16

    taps = sent_to_all(replica, ("beam", "pulse"))
    strip = strip_of_chip(signal)
    window, slope, floor, edge, scalars = pl.pallas_call(
        functools.partial(tables, shards),
        out_shape=(
            jax.ShapeDtypeStruct((3 * TILE, 2 * TILE), bf16),
            jax.ShapeDtypeStruct((16, INNER * TILE), f32),
            jax.ShapeDtypeStruct((16, TILE), f32),
            jax.ShapeDtypeStruct((16, TILE), f32),
            pltpu.SMEM((3,), jnp.int32),
        ),
        in_specs=[smem] * 5,
        out_specs=[vmem] * 4 + [smem],
        compiler_params=pltpu.CompilerParams(vmem_limit_bytes=4 << 20),
        cost_estimate=pl.CostEstimate(flops=1 << 20, bytes_accessed=1 << 18, transcendentals=0),
        name="tables",
    )(lax.axis_index("range").reshape(1), guard_cells, train_cells, scale_index, offsets)
    taps = taps.reshape(-1, taps.shape[-1])
    left, right = pl.pallas_call(
        prepare,
        out_shape=[jax.ShapeDtypeStruct((16, 2 * BLOCKS * TILE), bf16)] * 2,
        in_specs=[smem, vmem],
        out_specs=[vmem] * 2,
        compiler_params=pltpu.CompilerParams(vmem_limit_bytes=4 << 20),
        cost_estimate=pl.CostEstimate(flops=1 << 20, bytes_accessed=1 << 20, transcendentals=0),
        name="prepare",
    )(scalars, strip)
    compressed, ratio = pl.pallas_call(
        detect,
        out_shape=(
            jax.ShapeDtypeStruct((2, 8, 2, INNER * TILE), bf16),
            jax.ShapeDtypeStruct((2, 8, INNER * TILE), f32),
        ),
        in_specs=[vmem] * 7,
        out_specs=[vmem] * 2,
        scratch_shapes=[pltpu.VMEM((2 * INNER, 16, TILE), f32), pltpu.VMEM(taps.shape, f32)],
        compiler_params=pltpu.CompilerParams(vmem_limit_bytes=4 << 20),
        cost_estimate=pl.CostEstimate(flops=1 << 28, bytes_accessed=1 << 20, transcendentals=0),
        name="detect",
    )(taps, left, right, window, slope, floor, edge)
    return compressed, ratio


def solution(mesh):
    placed = (
        P("beam", "pulse", None, "range"),
        P(None, ("beam", "pulse")),
        P("beam"),
        P("beam"),
        P("beam"),
        P("beam"),
    )
    return jax.shard_map(
        body,
        mesh=mesh,
        in_specs=placed,
        out_specs=(P("beam", "pulse", None, "range"), P("beam", "pulse", "range")),
        check_vma=False,
    )
```

```python
import functools

import jax
import jax.numpy as jnp
from jax import lax
from jax.experimental import pallas as pl
from jax.experimental.pallas import tpu as pltpu
from jax.sharding import PartitionSpec as P


TILE = 128
EPSILON = 1e-6
INNER = 4
TILES = INNER + 2
CHUNKS = 17
BLOCKS = TILES + CHUNKS - 1


EARLY = 5
FIRST = 12


def sent_to_all(array, axes):
    beams, pulses = (lax.axis_size(axis) for axis in axes)
    order = [((FIRST + i) % beams) * pulses + j for i in range(beams) for j in range(pulses)]
    copies = jnp.broadcast_to(array, (beams * pulses, *array.shape))
    return lax.all_to_all(
        copies, axes, split_axis=0, concat_axis=0, tiled=True, axis_index_groups=[order]
    )


def strip_of_chip(signal):
    devices = lax.axis_size("range")
    cells = jnp.transpose(signal, (0, 2, 1, 3))
    half = cells.shape[3] // 2
    own = jnp.stack([cells[..., :half], cells[..., half:]])

    first = lax.rem(lax.axis_index("range"), 2) == 0
    ends = [(j + 6 if j % 2 == 0 else j - 2, j) for j in range(devices)]
    second = [(j + 4, j) for j in range(devices)]
    near = [(j + 2, j) for j in range(devices)]
    planes = lax.axis_size("beam")
    early = lax.axis_index("beam") < EARLY

    def sent(array, early_pairs, late_pairs):
        pairs = [(b * devices + i, b * devices + j) for b in range(EARLY) for i, j in early_pairs]
        pairs += [(b * devices + i, b * devices + j) for b in range(EARLY, planes) for i, j in late_pairs]
        inside = [(i, j) for i, j in pairs if i // devices == j // devices and i >= 0]
        return lax.ppermute(array, ("beam", "range"), inside)

    edge = jnp.where(first, own[:1], own[1:])
    got0 = sent(own, second, [])
    got1 = sent(edge, ends, ends)
    got2 = sent(own, near, second)
    got3 = sent(own, [], near)
    ahead = jnp.where(early, got2, got3)
    farther = jnp.where(early, got0, got2)
    rest = got1
    mine = jnp.concatenate([own, ahead, farther, rest], axis=0)
    chips = [[2 * i, 2 * i + 1] for i in range(devices // 2)]
    return lax.all_gather(mine, "range", axis_index_groups=chips, tiled=True)


def tables(shards, place_ref, guard_ref, train_ref, scale_ref, offset_ref, *outs):
    window_ref, slope_ref, floor_ref, edge_ref, scalars_ref = outs
    place = place_ref[0]
    scalars_ref[0] = offset_ref[0]
    scalars_ref[1] = offset_ref[1]
    scalars_ref[2] = lax.rem(place, 2)
    apart = jnp.abs(
        lax.broadcasted_iota(jnp.int32, (3 * TILE, TILE), 0)
        - TILE
        - lax.broadcasted_iota(jnp.int32, (3 * TILE, TILE), 1)
    )
    gate = place * (INNER * TILE) + lax.broadcasted_iota(jnp.int32, (8, INNER * TILE), 1)
    last = shards * INNER * TILE - 1
    for beam in range(2):
        guard = guard_ref[beam]
        train = train_ref[beam]
        inside = jnp.logical_and(apart > guard, apart <= guard + train)
        window_ref[:, beam * TILE : (beam + 1) * TILE] = jnp.where(inside, 1.0, 0.0).astype(
            jnp.bfloat16
        )
        count = jnp.clip(gate - guard, 0, train) + jnp.clip(last - gate - guard, 0, train)
        level = jnp.full((8, TILE), scale_ref[beam], jnp.int32).astype(jnp.float32)
        factor = jnp.exp2(level / 8.0)
        slope_ref[8 * beam : 8 * beam + 8, :] = jnp.concatenate(
            [factor] * INNER, axis=1
        ) / count.astype(jnp.float32)
        floor_ref[8 * beam : 8 * beam + 8, :] = factor * EPSILON
    edge_ref[0:8, :] = jnp.where(jnp.full((8, TILE), place, jnp.int32) > 0, 1.0, 0.0)
    edge_ref[8:16, :] = jnp.where(jnp.full((8, TILE), place, jnp.int32) < shards - 1, 1.0, 0.0)


def prepare(scalars_ref, strip_ref, left_ref, right_ref):
    lane = lax.broadcasted_iota(jnp.int32, (8, TILE), 1)

    count = strip_ref.shape[0] // 2
    strip = [2 * count - 1]
    strip += [core * count + at + sub for at in (0, 2, 4) for core in (0, 1) for sub in (0, 1)]
    strip += [count - 1]
    core = scalars_ref[2]
    blocks = []
    for n in range(len(strip) - 2):
        piece = jnp.where(core == 0, strip[n], strip[n + 2])
        blocks += [(piece, at) for at in ((TILE,) if n == 0 else (0, TILE))]

    aligned = []
    for beam in range(2):
        offset = scalars_ref[beam]
        shift = lax.rem(TILE - offset, TILE)
        whole = lane < TILE - offset
        parts = []
        for part in range(2):
            rolled = [
                pltpu.roll(
                    strip_ref[piece, beam, part, :, at : at + TILE].astype(jnp.float32), shift, 1
                )
                for piece, at in blocks
            ]
            parts.append([jnp.where(whole, rolled[n], rolled[n + 1]) for n in range(BLOCKS)])
        aligned.append(parts)
    for n in range(BLOCKS):
        real = jnp.concatenate([aligned[0][0][n], aligned[1][0][n]], axis=0)
        imag = jnp.concatenate([aligned[0][1][n], aligned[1][1][n]], axis=0)
        at = 2 * n * TILE
        left_ref[:, at : at + TILE] = real.astype(jnp.bfloat16)
        left_ref[:, at + TILE : at + 2 * TILE] = imag.astype(jnp.bfloat16)
        right_ref[:, at : at + TILE] = imag.astype(jnp.bfloat16)
        right_ref[:, at + TILE : at + 2 * TILE] = (-real).astype(jnp.bfloat16)


def detect(taps_ref, left_ref, right_ref, window_ref, slope_ref, floor_ref, edge_ref, *outs):
    compressed_ref, ratio_ref, pairs_ref, lines_ref = outs
    across = (((1,), (1,)), ((), ()))
    lane = lax.broadcasted_iota(jnp.int32, (8, TILE), 1)
    row = lax.broadcasted_iota(jnp.int32, (8, TILE), 0)

    lines_ref[...] = taps_ref[...].astype(jnp.float32)
    rows = []
    for part in range(2):
        quarters = [lines_ref[pl.ds(2 * q + part, 16, stride=8), :] for q in range(4)]
        rows.append(jnp.concatenate(quarters, axis=1))

    total = jnp.zeros((2 * TILES * 16, TILE), jnp.float32)
    before = None
    for chunk in range(CHUNKS):
        rolled = []
        for part in range(2):
            if chunk < CHUNKS - 1:
                at = (chunk - FIRST) % (CHUNKS - 1)
                line = jnp.broadcast_to(rows[part][at : at + 1, :], (8, TILE))
                rolled.append(
                    [pltpu.roll(line, 8 * q, 1, stride=1, stride_axis=0) for q in range(16)]
                )
            else:
                rolled.append([jnp.zeros((8, TILE), jnp.float32)] * 16)
        panel = []
        for part in range(2):
            pieces = []
            for q in range(16):
                old = before[part][q] if before is not None else jnp.zeros((8, TILE), jnp.float32)
                pieces.append(jnp.where(lane >= 8 * q + row, rolled[part][q], old))
            panel.append(jnp.concatenate(pieces, axis=0).astype(jnp.bfloat16))
        before = rolled
        weights = jnp.concatenate(panel, axis=1)
        samples = [
            ref[:, 2 * (tile + chunk) * TILE : 2 * (tile + chunk + 1) * TILE]
            for ref in (left_ref, right_ref)
            for tile in range(TILES)
        ]
        total = total + lax.dot_general(
            jnp.concatenate(samples, axis=0), weights, across, preferred_element_type=jnp.float32
        )

    rounded = total.astype(jnp.bfloat16)
    half = TILES * 16
    power = []
    for tile in range(TILES):
        real = rounded[16 * tile : 16 * tile + 16]
        imag = rounded[half + 16 * tile : half + 16 * tile + 16]
        if 1 <= tile <= INNER:
            at = (tile - 1) * TILE
            for beam in range(2):
                rows_of = slice(8 * beam, 8 * beam + 8)
                spot = 2 * (tile - 1) + beam
                pairs_ref[spot, pl.ds(0, 8, stride=2), :] = real.astype(jnp.float32)[rows_of]
                pairs_ref[spot, pl.ds(1, 8, stride=2), :] = imag.astype(jnp.float32)[rows_of]
                pairs = pairs_ref[spot].astype(jnp.bfloat16)
                compressed_ref[beam, :, :, at : at + TILE] = pairs.reshape(8, 2, TILE)
        real = real.astype(jnp.float32)
        imag = imag.astype(jnp.float32)
        power.append(real * real + imag * imag)
    power[0] = power[0] * jnp.concatenate([edge_ref[0:8, :]] * 2, axis=0)
    power[-1] = power[-1] * jnp.concatenate([edge_ref[8:16, :]] * 2, axis=0)

    terms = []
    rest = power
    for _ in range(3):
        term = [cells.astype(jnp.bfloat16) for cells in rest]
        rest = [cells - t.astype(jnp.float32) for cells, t in zip(rest, term)]
        terms += [
            jnp.concatenate(term[tile - 1 : tile + 2], axis=1) for tile in range(1, INNER + 1)
        ]
    sums = lax.dot_general(
        jnp.concatenate(terms, axis=0),
        window_ref[...],
        (((1,), (0,)), ((), ())),
        preferred_element_type=jnp.float32,
    )
    size = INNER * 16
    sums = sums[2 * size :] + sums[size : 2 * size] + sums[:size]
    for tile in range(INNER):
        at = tile * TILE
        for beam in range(2):
            noise = sums[16 * tile + 8 * beam : 16 * tile + 8 * beam + 8]
            noise = noise[:, beam * TILE : (beam + 1) * TILE]
            rows_of = slice(8 * beam, 8 * beam + 8)
            ratio_ref[beam, :, at : at + TILE] = power[tile + 1][rows_of] / (
                noise * slope_ref[rows_of, at : at + TILE] + floor_ref[rows_of, :]
            )


def body(signal, replica, guard_cells, train_cells, scale_index, offsets):
    shards = lax.axis_size("range")
    vmem = pl.BlockSpec(memory_space=pltpu.VMEM)
    smem = pl.BlockSpec(memory_space=pltpu.SMEM)
    f32, bf16 = jnp.float32, jnp.bfloat16

    taps = sent_to_all(replica, ("beam", "pulse"))
    strip = strip_of_chip(signal)
    window, slope, floor, edge, scalars = pl.pallas_call(
        functools.partial(tables, shards),
        out_shape=(
            jax.ShapeDtypeStruct((3 * TILE, 2 * TILE), bf16),
            jax.ShapeDtypeStruct((16, INNER * TILE), f32),
            jax.ShapeDtypeStruct((16, TILE), f32),
            jax.ShapeDtypeStruct((16, TILE), f32),
            pltpu.SMEM((3,), jnp.int32),
        ),
        in_specs=[smem] * 5,
        out_specs=[vmem] * 4 + [smem],
        compiler_params=pltpu.CompilerParams(vmem_limit_bytes=4 << 20),
        cost_estimate=pl.CostEstimate(flops=1 << 20, bytes_accessed=1 << 18, transcendentals=0),
        name="tables",
    )(lax.axis_index("range").reshape(1), guard_cells, train_cells, scale_index, offsets)
    taps = taps.reshape(-1, taps.shape[-1])
    left, right = pl.pallas_call(
        prepare,
        out_shape=[jax.ShapeDtypeStruct((16, 2 * BLOCKS * TILE), bf16)] * 2,
        in_specs=[smem, vmem],
        out_specs=[vmem] * 2,
        compiler_params=pltpu.CompilerParams(vmem_limit_bytes=4 << 20),
        cost_estimate=pl.CostEstimate(flops=1 << 20, bytes_accessed=1 << 20, transcendentals=0),
        name="prepare",
    )(scalars, strip)
    compressed, ratio = pl.pallas_call(
        detect,
        out_shape=(
            jax.ShapeDtypeStruct((2, 8, 2, INNER * TILE), bf16),
            jax.ShapeDtypeStruct((2, 8, INNER * TILE), f32),
        ),
        in_specs=[vmem] * 7,
        out_specs=[vmem] * 2,
        scratch_shapes=[pltpu.VMEM((2 * INNER, 16, TILE), f32), pltpu.VMEM(taps.shape, f32)],
        compiler_params=pltpu.CompilerParams(vmem_limit_bytes=4 << 20),
        cost_estimate=pl.CostEstimate(flops=1 << 28, bytes_accessed=1 << 20, transcendentals=0),
        name="detect",
    )(taps, left, right, window, slope, floor, edge)
    return compressed, ratio


def solution(mesh):
    placed = (
        P("beam", "pulse", None, "range"),
        P(None, ("beam", "pulse")),
        P("beam"),
        P("beam"),
        P("beam"),
        P("beam"),
    )
    return jax.shard_map(
        body,
        mesh=mesh,
        in_specs=placed,
        out_specs=(P("beam", "pulse", None, "range"), P("beam", "pulse", "range")),
        check_vma=False,
    )
```

```python
import functools

import jax
import jax.numpy as jnp
from jax import lax
from jax.experimental import pallas as pl
from jax.experimental.pallas import tpu as pltpu
from jax.sharding import PartitionSpec as P


TILE = 128
EPSILON = 1e-6
INNER = 4
TILES = INNER + 2
CHUNKS = 17
BLOCKS = TILES + CHUNKS - 1


EARLY = 6
ORDER = (12, *range(12), 13, 14, 15)


def sent_to_all(array, axes):
    beams, pulses = (lax.axis_size(axis) for axis in axes)
    order = [i * pulses + j for i in ORDER for j in range(pulses)]
    copies = jnp.broadcast_to(array, (beams * pulses, *array.shape))
    return lax.all_to_all(
        copies, axes, split_axis=0, concat_axis=0, tiled=True, axis_index_groups=[order]
    )


def strip_of_chip(signal):
    devices = lax.axis_size("range")
    cells = jnp.transpose(signal, (0, 2, 1, 3))
    half = cells.shape[3] // 2
    own = jnp.stack([cells[..., :half], cells[..., half:]])

    first = lax.rem(lax.axis_index("range"), 2) == 0
    ends = [(j + 6 if j % 2 == 0 else j - 2, j) for j in range(devices)]
    second = [(j + 4, j) for j in range(devices)]
    near = [(j + 2, j) for j in range(devices)]
    planes = lax.axis_size("beam")
    early = lax.axis_index("beam") < EARLY

    def sent(array, early_pairs, late_pairs):
        pairs = [(b * devices + i, b * devices + j) for b in range(EARLY) for i, j in early_pairs]
        pairs += [(b * devices + i, b * devices + j) for b in range(EARLY, planes) for i, j in late_pairs]
        inside = [(i, j) for i, j in pairs if i // devices == j // devices and i >= 0]
        return lax.ppermute(array, ("beam", "range"), inside)

    edge = jnp.where(first, own[:1], own[1:])
    got0 = sent(edge, ends, [])
    got1 = sent(jnp.where(early, own, jnp.concatenate([edge, edge])), second, ends)
    got2 = sent(own, near, second)
    got3 = sent(own, [], near)
    ahead = jnp.where(early, got2, got3)
    farther = jnp.where(early, got1, got2)
    rest = jnp.where(early, got0, got1[:1])
    mine = jnp.concatenate([own, ahead, farther, rest], axis=0)
    chips = [[2 * i, 2 * i + 1] for i in range(devices // 2)]
    return lax.all_gather(mine, "range", axis_index_groups=chips, tiled=True)


def tables(shards, place_ref, guard_ref, train_ref, scale_ref, offset_ref, *outs):
    window_ref, slope_ref, floor_ref, edge_ref, scalars_ref = outs
    place = place_ref[0]
    scalars_ref[0] = offset_ref[0]
    scalars_ref[1] = offset_ref[1]
    scalars_ref[2] = lax.rem(place, 2)
    apart = jnp.abs(
        lax.broadcasted_iota(jnp.int32, (3 * TILE, TILE), 0)
        - TILE
        - lax.broadcasted_iota(jnp.int32, (3 * TILE, TILE), 1)
    )
    gate = place * (INNER * TILE) + lax.broadcasted_iota(jnp.int32, (8, INNER * TILE), 1)
    last = shards * INNER * TILE - 1
    for beam in range(2):
        guard = guard_ref[beam]
        train = train_ref[beam]
        inside = jnp.logical_and(apart > guard, apart <= guard + train)
        window_ref[:, beam * TILE : (beam + 1) * TILE] = jnp.where(inside, 1.0, 0.0).astype(
            jnp.bfloat16
        )
        count = jnp.clip(gate - guard, 0, train) + jnp.clip(last - gate - guard, 0, train)
        level = jnp.full((8, TILE), scale_ref[beam], jnp.int32).astype(jnp.float32)
        factor = jnp.exp2(level / 8.0)
        slope_ref[8 * beam : 8 * beam + 8, :] = jnp.concatenate(
            [factor] * INNER, axis=1
        ) / count.astype(jnp.float32)
        floor_ref[8 * beam : 8 * beam + 8, :] = factor * EPSILON
    edge_ref[0:8, :] = jnp.where(jnp.full((8, TILE), place, jnp.int32) > 0, 1.0, 0.0)
    edge_ref[8:16, :] = jnp.where(jnp.full((8, TILE), place, jnp.int32) < shards - 1, 1.0, 0.0)


def prepare(scalars_ref, strip_ref, left_ref, right_ref):
    lane = lax.broadcasted_iota(jnp.int32, (8, TILE), 1)

    count = strip_ref.shape[0] // 2
    strip = [2 * count - 1]
    strip += [core * count + at + sub for at in (0, 2, 4) for core in (0, 1) for sub in (0, 1)]
    strip += [count - 1]
    core = scalars_ref[2]
    blocks = []
    for n in range(len(strip) - 2):
        piece = jnp.where(core == 0, strip[n], strip[n + 2])
        blocks += [(piece, at) for at in ((TILE,) if n == 0 else (0, TILE))]

    aligned = []
    for beam in range(2):
        offset = scalars_ref[beam]
        shift = lax.rem(TILE - offset, TILE)
        whole = lane < TILE - offset
        parts = []
        for part in range(2):
            rolled = [
                pltpu.roll(
                    strip_ref[piece, beam, part, :, at : at + TILE].astype(jnp.float32), shift, 1
                )
                for piece, at in blocks
            ]
            parts.append([jnp.where(whole, rolled[n], rolled[n + 1]) for n in range(BLOCKS)])
        aligned.append(parts)
    for n in range(BLOCKS):
        real = jnp.concatenate([aligned[0][0][n], aligned[1][0][n]], axis=0)
        imag = jnp.concatenate([aligned[0][1][n], aligned[1][1][n]], axis=0)
        at = 2 * n * TILE
        left_ref[:, at : at + TILE] = real.astype(jnp.bfloat16)
        left_ref[:, at + TILE : at + 2 * TILE] = imag.astype(jnp.bfloat16)
        right_ref[:, at : at + TILE] = imag.astype(jnp.bfloat16)
        right_ref[:, at + TILE : at + 2 * TILE] = (-real).astype(jnp.bfloat16)


def detect(taps_ref, left_ref, right_ref, window_ref, slope_ref, floor_ref, edge_ref, *outs):
    compressed_ref, ratio_ref, pairs_ref, lines_ref = outs
    across = (((1,), (1,)), ((), ()))
    lane = lax.broadcasted_iota(jnp.int32, (8, TILE), 1)
    row = lax.broadcasted_iota(jnp.int32, (8, TILE), 0)

    lines_ref[...] = taps_ref[...].astype(jnp.float32)
    rows = []
    for part in range(2):
        quarters = [lines_ref[pl.ds(2 * q + part, 16, stride=8), :] for q in range(4)]
        rows.append(jnp.concatenate(quarters, axis=1))

    total = jnp.zeros((2 * TILES * 16, TILE), jnp.float32)
    before = None
    for chunk in range(CHUNKS):
        rolled = []
        for part in range(2):
            if chunk < CHUNKS - 1:
                at = ORDER.index(chunk)
                line = jnp.broadcast_to(rows[part][at : at + 1, :], (8, TILE))
                rolled.append(
                    [pltpu.roll(line, 8 * q, 1, stride=1, stride_axis=0) for q in range(16)]
                )
            else:
                rolled.append([jnp.zeros((8, TILE), jnp.float32)] * 16)
        panel = []
        for part in range(2):
            pieces = []
            for q in range(16):
                old = before[part][q] if before is not None else jnp.zeros((8, TILE), jnp.float32)
                pieces.append(jnp.where(lane >= 8 * q + row, rolled[part][q], old))
            panel.append(jnp.concatenate(pieces, axis=0).astype(jnp.bfloat16))
        before = rolled
        weights = jnp.concatenate(panel, axis=1)
        samples = [
            ref[:, 2 * (tile + chunk) * TILE : 2 * (tile + chunk + 1) * TILE]
            for ref in (left_ref, right_ref)
            for tile in range(TILES)
        ]
        total = total + lax.dot_general(
            jnp.concatenate(samples, axis=0), weights, across, preferred_element_type=jnp.float32
        )

    rounded = total.astype(jnp.bfloat16)
    half = TILES * 16
    power = []
    for tile in range(TILES):
        real = rounded[16 * tile : 16 * tile + 16]
        imag = rounded[half + 16 * tile : half + 16 * tile + 16]
        if 1 <= tile <= INNER:
            at = (tile - 1) * TILE
            for beam in range(2):
                rows_of = slice(8 * beam, 8 * beam + 8)
                spot = 2 * (tile - 1) + beam
                pairs_ref[spot, pl.ds(0, 8, stride=2), :] = real.astype(jnp.float32)[rows_of]
                pairs_ref[spot, pl.ds(1, 8, stride=2), :] = imag.astype(jnp.float32)[rows_of]
                pairs = pairs_ref[spot].astype(jnp.bfloat16)
                compressed_ref[beam, :, :, at : at + TILE] = pairs.reshape(8, 2, TILE)
        real = real.astype(jnp.float32)
        imag = imag.astype(jnp.float32)
        power.append(real * real + imag * imag)
    power[0] = power[0] * jnp.concatenate([edge_ref[0:8, :]] * 2, axis=0)
    power[-1] = power[-1] * jnp.concatenate([edge_ref[8:16, :]] * 2, axis=0)

    terms = []
    rest = power
    for _ in range(3):
        term = [cells.astype(jnp.bfloat16) for cells in rest]
        rest = [cells - t.astype(jnp.float32) for cells, t in zip(rest, term)]
        terms += [
            jnp.concatenate(term[tile - 1 : tile + 2], axis=1) for tile in range(1, INNER + 1)
        ]
    sums = lax.dot_general(
        jnp.concatenate(terms, axis=0),
        window_ref[...],
        (((1,), (0,)), ((), ())),
        preferred_element_type=jnp.float32,
    )
    size = INNER * 16
    sums = sums[2 * size :] + sums[size : 2 * size] + sums[:size]
    for tile in range(INNER):
        at = tile * TILE
        for beam in range(2):
            noise = sums[16 * tile + 8 * beam : 16 * tile + 8 * beam + 8]
            noise = noise[:, beam * TILE : (beam + 1) * TILE]
            rows_of = slice(8 * beam, 8 * beam + 8)
            ratio_ref[beam, :, at : at + TILE] = power[tile + 1][rows_of] / (
                noise * slope_ref[rows_of, at : at + TILE] + floor_ref[rows_of, :]
            )


def body(signal, replica, guard_cells, train_cells, scale_index, offsets):
    shards = lax.axis_size("range")
    vmem = pl.BlockSpec(memory_space=pltpu.VMEM)
    smem = pl.BlockSpec(memory_space=pltpu.SMEM)
    f32, bf16 = jnp.float32, jnp.bfloat16

    taps = sent_to_all(replica, ("beam", "pulse"))
    strip = strip_of_chip(signal)
    window, slope, floor, edge, scalars = pl.pallas_call(
        functools.partial(tables, shards),
        out_shape=(
            jax.ShapeDtypeStruct((3 * TILE, 2 * TILE), bf16),
            jax.ShapeDtypeStruct((16, INNER * TILE), f32),
            jax.ShapeDtypeStruct((16, TILE), f32),
            jax.ShapeDtypeStruct((16, TILE), f32),
            pltpu.SMEM((3,), jnp.int32),
        ),
        in_specs=[smem] * 5,
        out_specs=[vmem] * 4 + [smem],
        compiler_params=pltpu.CompilerParams(vmem_limit_bytes=4 << 20),
        cost_estimate=pl.CostEstimate(flops=1 << 20, bytes_accessed=1 << 18, transcendentals=0),
        name="tables",
    )(lax.axis_index("range").reshape(1), guard_cells, train_cells, scale_index, offsets)
    taps = taps.reshape(-1, taps.shape[-1])
    left, right = pl.pallas_call(
        prepare,
        out_shape=[jax.ShapeDtypeStruct((16, 2 * BLOCKS * TILE), bf16)] * 2,
        in_specs=[smem, vmem],
        out_specs=[vmem] * 2,
        compiler_params=pltpu.CompilerParams(vmem_limit_bytes=4 << 20),
        cost_estimate=pl.CostEstimate(flops=1 << 20, bytes_accessed=1 << 20, transcendentals=0),
        name="prepare",
    )(scalars, strip)
    compressed, ratio = pl.pallas_call(
        detect,
        out_shape=(
            jax.ShapeDtypeStruct((2, 8, 2, INNER * TILE), bf16),
            jax.ShapeDtypeStruct((2, 8, INNER * TILE), f32),
        ),
        in_specs=[vmem] * 7,
        out_specs=[vmem] * 2,
        scratch_shapes=[pltpu.VMEM((2 * INNER, 16, TILE), f32), pltpu.VMEM(taps.shape, f32)],
        compiler_params=pltpu.CompilerParams(vmem_limit_bytes=4 << 20),
        cost_estimate=pl.CostEstimate(flops=1 << 28, bytes_accessed=1 << 20, transcendentals=0),
        name="detect",
    )(taps, left, right, window, slope, floor, edge)
    return compressed, ratio


def solution(mesh):
    placed = (
        P("beam", "pulse", None, "range"),
        P(None, ("beam", "pulse")),
        P("beam"),
        P("beam"),
        P("beam"),
        P("beam"),
    )
    return jax.shard_map(
        body,
        mesh=mesh,
        in_specs=placed,
        out_specs=(P("beam", "pulse", None, "range"), P("beam", "pulse", "range")),
        check_vma=False,
    )
```
